256 devices in a mesh: tm: 8 (over z), node: 32 (over x, y, core).
Axes of the slice: x: 4, y: 4, z: 8, core: 2. Of those that a mesh axis runs over, the one named last changes fastest.
Arguments:
- memory: float32 [16384, 256], P('node'), may hold values from -6 to 6
- src_slot: int32 [8, 32, 512], P('tm', 'node'), may hold values from 0 to 4095, as said below
- dst_slot: int32 [8, 32, 512], P('tm', 'node'), may hold values from 0 to 4095, as said below
- event_time: float32 [8, 32, 512], P('tm', 'node'), may hold values from 0 to 200
- touched_rows: int32 [8, 32, 32, 128], P('tm', 'node'), may hold values from 0 to 511, as said below
- time_freq: float32 [128], replicated, may hold values from 0.01 to 1
- msg_weight: bfloat16 [640, 256], replicated, may hold values from -0.25 to 0.25
- msg_bias: float32 [256], replicated, may hold values from -3 to 3
- gate_weight: bfloat16 [256, 512], replicated, may hold values from -0.375 to 0.375
- update_bias: float32 [256], replicated, may hold values from -5 to 1
Outputs:
- period_memory: float32 [8, 16384, 256], P('tm', 'node')
The draws below stay inside these ranges and needn't reach their ends.
Inputs may be any that keep to these rules, and one draw needn't show every extreme that they name: touched_rows[t, o, b] holds 128 distinct rows among the 512 rows that owner o keeps. `src_slot`: slot s of event block b in period t stands for node (s // 128) * 512 + touched_rows[t, s // 128, b, s % 128]. `dst_slot`: read as src_slot.
All inputs are finite; a program needn't handle non-finite values.
Results may differ from the reference program's by a relative error of at most 0.0019.
Values may be sent and summed in bfloat16 or wider, within the bound.
A program may use at most 64 MiB of HBM per device.

```python
import math
import jax
import jax.numpy as jnp
from jax import lax

MW = 256
TW = 128
CAP = 128
NODE_DEV = 512
EV_DEV = 512
PERIODS = 8
BLOCKS = 32
NODES = 16384


def slot_counts(base_key):
    count_key, owner_key, request_key = jax.random.split(jax.random.fold_in(base_key, 7), 3)
    counts = jax.random.randint(count_key, (PERIODS, BLOCKS, BLOCKS), CAP // 4, CAP + 1)
    requester = jnp.arange(BLOCKS)[None, None, :]
    full_one = jax.random.randint(owner_key, (PERIODS, BLOCKS, 1), 0, BLOCKS)
    counts = jnp.where(requester == full_one, CAP, counts)
    full_all = jax.random.randint(request_key, (PERIODS, 1, 1), 0, BLOCKS)
    counts = jnp.where(requester == full_all, CAP, counts)
    return counts


def event_slots(base_key, salt_value):
    counts = slot_counts(base_key)
    first_key, second_key, turn_key, place_key = jax.random.split(jax.random.fold_in(base_key, salt_value), 4)
    shape = (PERIODS, BLOCKS, EV_DEV)
    first_pick = jax.random.randint(first_key, shape, 0, BLOCKS)
    second = jax.random.randint(second_key, shape, 0, BLOCKS)
    rotation = jax.random.randint(turn_key, (PERIODS, 1, 1), 0, BLOCKS)
    owner_id = (jnp.minimum(first_pick, second) + rotation) % BLOCKS
    period_ids = jnp.arange(PERIODS)[:, None, None]
    block_ids = jnp.arange(BLOCKS)[None, :, None]
    limits = counts[period_ids, owner_id, block_ids]
    position = jax.random.randint(place_key, shape, 0, limits)
    return (owner_id * CAP + position).astype(jnp.int32)


def draw_src_slot(key, part):
    return event_slots(key, 21)


def draw_dst_slot(key, part):
    return event_slots(key, 22)


def draw_touched_rows(key, part):
    random_bits = jax.random.randint(jax.random.fold_in(key, 11), (PERIODS, BLOCKS, BLOCKS, NODE_DEV), 0, 1 << 16)
    scores = random_bits * NODE_DEV + jnp.arange(NODE_DEV)
    ordering = jnp.argsort(scores, axis=-1)
    return ordering[..., :CAP].astype(jnp.int32)


def steps_of(stream_key, shape, cuts, smallest, high):
    def one(dim, parts):
        heights = jax.random.uniform(jax.random.fold_in(jax.random.fold_in(stream_key, 6), dim), (parts,), jnp.float32, smallest / len(cuts), high / len(cuts))
        return jnp.repeat(jnp.exp(heights), shape[dim] // parts).reshape((-1,) + (1,) * (len(shape) - dim - 1))

    gain = one(*cuts[0])
    for cut in cuts[1:]:
        gain = gain * one(*cut)
    return gain


def gaussian(own_key, dims, spread, most, cuts=(), held_as=jnp.bfloat16):
    drawn = spread * jax.random.normal(own_key, dims, jnp.float32)
    if cuts:
        drawn = drawn * steps_of(own_key, dims, cuts, -0.22, 0.18)
    return jnp.clip(drawn, -most, most).astype(held_as)


def setup_inputs(seed: int = 0) -> dict:
    splits = jax.random.split(jax.random.key(seed), 11)
    memory = gaussian(splits[0], (NODES, MW), 1.0, 6.0, ((0, 32),), jnp.float32)
    src_slot = draw_src_slot(jax.random.fold_in(splits[10], 71), 0)
    dst_slot = draw_dst_slot(jax.random.fold_in(splits[10], 71), 0)
    event_time = jnp.clip(200.0 * jax.random.uniform(splits[3], (PERIODS, BLOCKS, EV_DEV), jnp.float32) ** steps_of(splits[3], (PERIODS, BLOCKS, EV_DEV), ((0, 8), (1, 32)), -0.2, 0.2), 0.0, 200.0)
    touched_rows = draw_touched_rows(jax.random.fold_in(splits[10], 71), 0)
    time_freq = jnp.clip(jnp.exp(jax.random.uniform(splits[5], (TW,), jnp.float32, math.log(0.01), math.log(1.0))), 0.01, 1.0)
    msg_weight = gaussian(splits[6], (2 * MW + TW, MW), (2 * MW + TW) ** -0.5, 0.25)
    msg_bias = gaussian(splits[7], (MW,), 0.5, 3.0, (), jnp.float32)
    gate_weight = gaussian(splits[8], (MW, 2 * MW), MW ** -0.5, 0.375)
    update_bias = jnp.clip(jax.random.uniform(splits[9], (MW,), jnp.float32, -5.0, 1.0), -5.0, 1.0)
    return {"memory": memory, "src_slot": src_slot, "dst_slot": dst_slot, "event_time": event_time, "touched_rows": touched_rows, "time_freq": time_freq, "msg_weight": msg_weight, "msg_bias": msg_bias, "gate_weight": gate_weight, "update_bias": update_bias}


def reference(memory, src_slot, dst_slot, event_time, touched_rows, time_freq, msg_weight, msg_bias, gate_weight, update_bias):
    capacity = touched_rows.shape[3]
    total_nodes = memory.shape[0]
    node_rows = total_nodes // src_slot.shape[1]
    breadth = memory.shape[1]
    rounded = lax.optimization_barrier(memory.astype(jnp.bfloat16)).astype(memory.dtype)
    weight_wide = msg_weight.astype(memory.dtype)
    gate_wide = gate_weight.astype(memory.dtype)

    def node_lookup(slot_ids, slot_table):
        owner_id = (slot_ids // capacity).astype(jnp.int32)
        position = (slot_ids % capacity).astype(jnp.int32)
        return slot_table[owner_id, position] + owner_id * node_rows

    def one_block(running, pieces):
        totals, counts = running
        sources, targets, event_times, slot_table = pieces
        src_node = node_lookup(sources, slot_table)
        dst_node = node_lookup(targets, slot_table)
        from_rows = rounded[src_node]
        to_rows = rounded[dst_node]
        encoding = jnp.cos(event_times[:, None] * time_freq[None, :])
        encoding = lax.optimization_barrier(encoding.astype(jnp.bfloat16)).astype(memory.dtype)
        inputs = jnp.concatenate([
            jnp.concatenate([from_rows, to_rows, encoding], 1),
            jnp.concatenate([to_rows, from_rows, encoding], 1)], 0)
        messages = jax.nn.relu(jnp.dot(inputs, weight_wide, precision=lax.Precision.HIGHEST) + msg_bias)
        all_nodes = jnp.concatenate([src_node, dst_node])
        totals = totals.at[all_nodes].add(messages)
        counts = counts.at[all_nodes].add(jnp.ones(all_nodes.shape, memory.dtype))
        return (totals, counts), None

    def one_period(memory_state, period_data):
        sources, targets, event_times, row_lists = period_data
        zero_sums = (jnp.zeros_like(memory), jnp.zeros((total_nodes,), memory.dtype))
        (totals, counts), unused = lax.scan(one_block, zero_sums, (sources, targets, event_times, jnp.swapaxes(row_lists, 0, 1)))
        mean_msg = totals / jnp.maximum(counts, 1.0)[:, None]
        mean_msg = lax.optimization_barrier(mean_msg.astype(jnp.bfloat16)).astype(memory.dtype)
        gate_terms = jnp.dot(mean_msg, gate_wide, precision=lax.Precision.HIGHEST)
        update = jax.nn.sigmoid(gate_terms[:, :breadth] + update_bias)
        candidate = jnp.tanh(gate_terms[:, breadth:])
        touched = (counts > 0.0)[:, None]
        keep_rate = jnp.where(touched, 1.0 - update, 1.0)
        write_term = jnp.where(touched, update * candidate, 0.0)
        updated = keep_rate * memory_state + write_term
        return updated, updated

    final_state, history = lax.scan(one_period, memory, (src_slot, dst_slot, event_time, touched_rows))
    return history
```

```python
import functools

import jax
import jax.numpy as jnp
from jax import lax
from jax.experimental import pallas as pl
from jax.experimental.pallas import tpu as pltpu
from jax.sharding import PartitionSpec as P

MESH = pl.DeviceIdType.MESH
F32 = jnp.float32
BF16 = jnp.bfloat16
NT = (((1,), (1,)), ((), ()))
NN = (((1,), (0,)), ((), ()))

PERIODS = 8
OWNERS = 32
ROWS = 512
WIDTH = 256
TERMS = 1024
SHARE = ROWS // PERIODS
BLOCKS = PERIODS * OWNERS
CHUNK = 256


def dot(a, b, dims=NN):
    return lax.dot_general(a, b, dims, preferred_element_type=F32)


def iota(shape, dim):
    return lax.broadcasted_iota(jnp.int32, shape, dim)


def where01(mask):
    return jnp.where(mask, 1.0, 0.0).astype(BF16)


def sorted_terms(slots, times, lists):
    lane = iota((TERMS, 128), 1)
    owner = slots >> 7
    table = jnp.concatenate([(lists - 256).astype(F32), jnp.zeros((128 - OWNERS, 128), F32)], 0)
    per_owner = dot(where01(owner == lane), table.astype(BF16))
    picked = jnp.where((slots & 127) == lane, per_owner, 0.0).astype(BF16)
    ones = jnp.ones((128, 128), BF16)
    row = dot(picked, ones).astype(jnp.int32) + 256
    node = owner * ROWS + row
    bucket = (node >> 6).astype(F32)
    rest = (node & 63).astype(F32)
    eighth = jnp.full((8, 128), 1.0 / 128.0, BF16)
    bucket_row = dot(eighth, bucket.astype(BF16), NT)
    rest_row = dot(eighth, rest.astype(BF16), NT)
    key_col = bucket * TERMS + iota((TERMS, 128), 0).astype(F32)
    key_row = bucket_row * TERMS + iota((8, TERMS), 1).astype(F32)
    below = jnp.zeros((TERMS, 128), F32)
    for q in range(8):
        part = jnp.broadcast_to(key_row[0:1, 128 * q : 128 * (q + 1)], (TERMS, 128))
        below = below + jnp.where(part < key_col, 1.0, 0.0)
    place = dot(below.astype(BF16), ones).astype(jnp.int32)
    half = TERMS // 2
    other_bucket = jnp.concatenate([bucket_row[:, half:], bucket_row[:, :half]], 1)
    other_rest = jnp.concatenate([rest_row[:, half:], rest_row[:, :half]], 1)
    time = jnp.broadcast_to(jnp.concatenate([times, times], 1), (8, TERMS))
    t1 = time.astype(BF16).astype(F32)
    t2 = (time - t1).astype(BF16).astype(F32)
    t3 = time - t1 - t2
    which = iota((8, TERMS), 0)
    meta = jnp.zeros((8, TERMS), F32)
    for k, piece in enumerate((bucket_row, rest_row, other_bucket, other_rest, t1, t2, t3)):
        meta = jnp.where(which == k, piece, meta)
    meta = meta.astype(BF16)
    rows = []
    for q in range(8):
        out = dot(meta, where01(place == lane + 128 * q))
        whole = out.astype(jnp.int32)
        own = whole[0:1] * 64 + whole[1:2]
        other = whole[2:3] * 64 + whole[3:4]
        rows.append(((own << 14) | other, out[4:5] + out[5:6] + out[6:7]))
    return rows


class Gather:
    OPS = 36

    def __init__(self, ref, top, bottom, full, first, base, sems, at):
        self.ref, self.top, self.bottom, self.full = ref, top, bottom, full
        self.first, self.base, self.sems, self.at = first, base, sems, at
        self.started = {}

    def node(self, du, dv, flip=False):
        t, x, y, c = self.at
        dx, dy = (du, dv) if self.first == 0 else (dv, du)
        core = 1 - c if flip else c
        return (lax.rem(x + dx + 4, 4) * 4 + lax.rem(y + dy + 4, 4)) * 2 + core

    def start(self, op, du, dv, part, to):
        piece = self.ref.at[(self.node(du, dv),) + part]
        copy = pltpu.make_async_remote_copy(
            src_ref=piece,
            dst_ref=piece,
            send_sem=self.sems.at[0, self.base + op],
            recv_sem=self.sems.at[1, self.base + op],
            device_id=(self.at[0], to),
            device_id_type=MESH,
        )
        copy.start()
        self.started[op] = copy

    def wait(self, op):
        self.started[op].wait_recv()

    def share(self, k, du, dv):
        self.start(20 + k, du, dv, self.full, self.node(0, 0, True))

    def second(self, i, du):
        self.start(4 + 4 * i, du, 0, self.full, self.node(0, 1))
        self.start(5 + 4 * i, du, 0, self.full, self.node(0, -1))
        self.share(4 * i, du, 0)

    def begin(self):
        self.start(0, 0, 0, self.full, self.node(1, 0))
        self.start(1, 0, 0, self.full, self.node(-1, 0))
        self.second(0, 0)

    def near(self):
        self.wait(0)
        self.start(2, -1, 0, self.top, self.node(1, 0))
        self.second(1, -1)
        self.wait(1)
        self.start(3, 1, 0, self.bottom, self.node(-1, 0))
        self.second(2, 1)

    def far(self):
        self.wait(2)
        self.wait(3)
        self.second(3, 2)

    def column_near(self, i, du):
        self.wait(4 + 4 * i)
        self.start(6 + 4 * i, du, -1, self.top, self.node(0, 1))
        self.share(4 * i + 1, du, -1)
        self.wait(5 + 4 * i)
        self.start(7 + 4 * i, du, 1, self.bottom, self.node(0, -1))
        self.share(4 * i + 2, du, 1)

    def column_far(self, i, du):
        self.wait(6 + 4 * i)
        self.wait(7 + 4 * i)
        self.share(4 * i + 3, du, 2)

    def finish(self):
        for k in range(16):
            self.wait(20 + k)
        for copy in self.started.values():
            copy.wait_send()


def spread_kernel(
    memory, slots, times, lists, table, meta, time, block_lists, sems, list_sems, share_sems
):
    t = lax.axis_index("tm")
    o = lax.axis_index("node")
    x, y, c = o // 8, lax.rem(o // 2, 4), lax.rem(o, 2)
    at = (t, x, y, c)
    barrier = pltpu.get_barrier_semaphore()

    def greet(k, carry):
        pl.semaphore_signal(
            barrier, inc=1, device_id=(t, lax.rem(o + k, OWNERS)), device_id_type=MESH
        )
        return carry

    def greet_periods(k, carry):
        pl.semaphore_signal(
            barrier, inc=1, device_id=(lax.rem(t + k, PERIODS), o), device_id_type=MESH
        )
        return carry

    lax.fori_loop(1, OWNERS, greet, 0)
    lax.fori_loop(1, PERIODS, greet_periods, 0)
    table[pl.ds(o, 1)] = memory[...].astype(BF16)[None]
    block_lists[pl.ds(o, 1)] = lists[pl.ds(o, 1)]
    pl.semaphore_wait(barrier, OWNERS - 1 + PERIODS - 1)

    def list_copy(k):
        to = lax.rem(o + k, OWNERS)
        return pltpu.make_async_remote_copy(
            src_ref=lists.at[to],
            dst_ref=block_lists.at[o],
            send_sem=list_sems.at[0, k],
            recv_sem=list_sems.at[1, k],
            device_id=(t, to),
            device_id_type=MESH,
        )

    def start_list(k, carry):
        list_copy(k).start()
        return carry

    def wait_list(k, carry):
        list_copy(k).wait()
        return carry

    lax.fori_loop(1, OWNERS, start_list, 0)

    def halves(ref, size, step, first, base):
        return Gather(
            ref,
            (pl.ds(step, size // 2),),
            (pl.ds(step + size // 2, size // 2),),
            (pl.ds(step, size),),
            first,
            base,
            sems,
            at,
        )

    n = Gather.OPS
    big = (halves(table, 256, 0, 0, 0), halves(table, 256, 256, 1, n))
    small = (halves(meta, 8, 0, 0, 2 * n), halves(time, 8, 0, 1, 3 * n))
    columns = ((0, 0), (1, -1), (2, 1), (3, 2))
    for g in big:
        g.begin()
    lax.fori_loop(1, OWNERS, wait_list, 0)
    rows = sorted_terms(slots[...], times[...], block_lists[:, 0, :])
    for q, (meta_row, time_row) in enumerate(rows):
        meta[o, t, pl.ds(q, 1), :] = meta_row
        time[o, t, pl.ds(q, 1), :] = time_row
    for g in big:
        g.near()
    sent = []
    for k in range(1, PERIODS):
        for j, ref in enumerate((meta, time)):
            copy = pltpu.make_async_remote_copy(
                src_ref=ref.at[o, t],
                dst_ref=ref.at[o, t],
                send_sem=share_sems.at[0, j, k],
                recv_sem=share_sems.at[1, j, k],
                device_id=(lax.rem(t + k, PERIODS), o),
                device_id_type=MESH,
            )
            copy.start()
            sent.append(copy)
    for g in big:
        g.far()
    for g in big:
        g.column_near(*columns[0])
    for copy in sent:
        copy.wait()
    for g in small:
        g.begin()
    for col in columns[1:3]:
        for g in big:
            g.column_near(*col)
    for g in small:
        g.near()
    for g in big:
        g.column_near(*columns[3])
    for g in small:
        g.far()
    for col in columns[:3]:
        for g in big:
            g.column_far(*col)
        for g in small:
            g.column_near(*col)
    for g in big:
        g.column_far(*columns[3])
    for g in small:
        g.column_near(*columns[3])
    for col in columns:
        for g in small:
            g.column_far(*col)
    for g in big + small:
        g.finish()


def spread(memory, slots, times, lists):
    return pl.pallas_call(
        spread_kernel,
        out_shape=(
            jax.ShapeDtypeStruct((OWNERS, ROWS, WIDTH), BF16),
            jax.ShapeDtypeStruct((OWNERS, PERIODS, 8, 128), jnp.int32),
            jax.ShapeDtypeStruct((OWNERS, PERIODS, 8, 128), F32),
        ),
        in_specs=[pl.BlockSpec(memory_space=pltpu.VMEM)] * 4,
        out_specs=[pl.BlockSpec(memory_space=pltpu.VMEM)] * 3,
        scratch_shapes=[
            pltpu.VMEM((OWNERS, 1, 128), jnp.int32),
            pltpu.SemaphoreType.DMA((2, 4 * Gather.OPS)),
            pltpu.SemaphoreType.DMA((2, OWNERS)),
            pltpu.SemaphoreType.DMA((2, 2, PERIODS)),
        ],
        compiler_params=pltpu.CompilerParams(
            collective_id=0, has_side_effects=True, vmem_limit_bytes=40 * 2**20
        ),
        name="spread",
    )(memory, slots, times, lists)


def message_kernel(
    table, meta, time, freq, weight, bias, totals, counts,
    wide, window, window_time, pieces, rows_v, rows_s, index_v, index_s, gathered, sem,
):
    bucket = lax.axis_index("node") * PERIODS + lax.axis_index("tm")

    def widen(i, carry):
        at = pl.multiple_of(i * 256, 256)
        wide[pl.ds(at, 256), :] = table[pl.ds(at, 256), :].astype(F32)
        return carry

    lax.fori_loop(0, OWNERS * ROWS // 256, widen, 0)
    totals[...] = jnp.zeros_like(totals)
    counts[...] = jnp.zeros_like(counts)
    start_parts, end_parts = [], []
    for i in range(8):
        own = meta[pl.ds(32 * i, 32)] >> 20
        start_parts.append(jnp.sum(jnp.where(own < bucket, 1.0, 0.0), axis=1))
        end_parts.append(jnp.sum(jnp.where(own <= bucket, 1.0, 0.0), axis=1))
    ones_row = jnp.ones((8, 128), BF16)
    start = dot(ones_row, jnp.concatenate(start_parts, 0).astype(BF16), NT)
    end = dot(ones_row, jnp.concatenate(end_parts, 0).astype(BF16), NT)
    upper = where01(iota((BLOCKS, BLOCKS), 0) < iota((BLOCKS, BLOCKS), 1))
    own_rows = wide[pl.ds(pl.multiple_of(bucket * SHARE, SHARE), SHARE), :].astype(BF16)
    own_rows = jnp.concatenate([own_rows, jnp.zeros((128 - SHARE, WIDTH), BF16)], 0)
    ones_wide = jnp.ones((8, BLOCKS), BF16)
    ones_col = jnp.ones((BLOCKS, 128), BF16)
    freqs = jnp.broadcast_to(freq[...], (CHUNK, 128))
    biases = jnp.broadcast_to(bias[...], (CHUNK, WIDTH))
    longest = jnp.max(end - start)

    def one_round(r, carry):
        begin = start + (r * 128).astype(F32)
        size = jnp.clip(end - begin, 0.0, 128.0)
        before = dot(size.astype(BF16), upper)
        which = iota((8, BLOCKS), 0)
        begin_i = begin.astype(jnp.int32)
        rows_v[...] = jnp.where(which == 0, begin_i, (before + size).astype(jnp.int32))
        copy = pltpu.make_async_copy(rows_v, rows_s, sem)
        copy.start()
        copy.wait()
        total = rows_s[1, BLOCKS - 1]

        def fetch(i, carry):
            for u in range(8):
                b = i * 8 + u
                at = rows_s[0, b] >> 7
                a0 = jnp.minimum(at, 7)
                a1 = jnp.minimum(at + 1, 7)
                window[b, 0] = meta[b, a0]
                window[b, 1] = meta[b, a1]
                window_time[b, 0] = time[b, a0]
                window_time[b, 1] = time[b, a1]
            return carry

        lax.fori_loop(0, BLOCKS // 8, fetch, 0)
        for j in range(2):
            m = window[:, j, :]
            w = window_time[:, j, :]
            period = iota((BLOCKS, 128), 0) & 7
            seg = period * SHARE + ((m >> 14) & 63) - 256
            t1 = w.astype(BF16).astype(F32)
            t2 = (w - t1).astype(BF16).astype(F32)
            t3 = w - t1 - t2
            for k, piece in enumerate(
                (seg.astype(F32), ((m >> 6) & 255).astype(F32), (m & 63).astype(F32), t1, t2, t3)
            ):
                pieces[:, 256 * k + 128 * j : 256 * k + 128 * (j + 1)] = piece.astype(BF16)
        offset = (begin_i & 127).astype(F32) - before

        def one_chunk(ch, carry):
            p = (ch * CHUNK).astype(F32) + iota((CHUNK, BLOCKS), 0).astype(F32)
            low = jnp.broadcast_to(before[0:1], (CHUNK, BLOCKS))
            high = low + jnp.broadcast_to(size[0:1], (CHUNK, BLOCKS))
            hit = (low <= p) & (p < high)
            shift = jnp.sum(
                jnp.where(hit, jnp.broadcast_to(offset[0:1], (CHUNK, BLOCKS)), 0.0),
                axis=1,
                keepdims=True,
            )
            found = dot(where01(hit), pieces[...])
            here = (p + shift) == iota((CHUNK, BLOCKS), 1).astype(F32)
            chosen = [
                jnp.where(here, found[:, 256 * k : 256 * (k + 1)], 0.0).astype(BF16)
                for k in range(6)
            ]
            other = dot(ones_wide, chosen[1], NT) * 64.0 + dot(ones_wide, chosen[2], NT)
            index_v[...] = other.astype(jnp.int32)
            copy = pltpu.make_async_copy(index_v, index_s, sem)
            copy.start()
            seg_row = dot(ones_wide, chosen[0], NT) + 256.0
            lane_p = (ch * CHUNK + iota((8, CHUNK), 1)).astype(F32)
            seg_row = jnp.where(lane_p < total.astype(F32), seg_row, -1.0)
            seg_col = dot(chosen[0], ones_col).astype(jnp.int32) + 256
            own_hot = where01((seg_col & 63) == iota((CHUNK, 128), 1))
            own = dot(own_hot, own_rows).astype(BF16)
            moment = dot(chosen[3], ones_col) + dot(chosen[4], ones_col) + dot(chosen[5], ones_col)
            encoding = jnp.cos(moment * freqs).astype(BF16)
            part = dot(own, weight[pl.ds(0, WIDTH), :]) + dot(
                encoding, weight[pl.ds(2 * WIDTH, 128), :]
            )
            seg_hot = where01(
                iota((ROWS, CHUNK), 0).astype(F32) == jnp.broadcast_to(seg_row[0:1], (ROWS, CHUNK))
            )
            copy.wait()

            def pick(i, carry):
                for u in range(8):
                    q = i * 8 + u
                    gathered[pl.ds(q, 1), :] = wide[pl.ds(index_s[0, q], 1), :]
                return carry

            lax.fori_loop(0, CHUNK // 8, pick, 0)
            part = part + dot(gathered[...].astype(BF16), weight[pl.ds(WIDTH, WIDTH), :])
            message = jnp.maximum(part + biases, 0.0)
            upper_part = message.astype(BF16)
            lower_part = (message - upper_part.astype(F32)).astype(BF16)
            totals[...] += dot(seg_hot, upper_part) + dot(seg_hot, lower_part)
            counts[...] += dot(seg_hot, ones_col)
            return carry

        lax.fori_loop(0, (total + CHUNK - 1) // CHUNK, one_chunk, 0)
        return carry

    rounds = (longest.astype(jnp.int32) + 127) // 128
    lax.fori_loop(0, rounds, one_round, 0)


def messages(table, meta, time, freq, weight, bias):
    return pl.pallas_call(
        message_kernel,
        out_shape=(
            jax.ShapeDtypeStruct((ROWS, WIDTH), F32),
            jax.ShapeDtypeStruct((ROWS, 128), F32),
        ),
        in_specs=[pl.BlockSpec(memory_space=pltpu.VMEM)] * 6,
        out_specs=[pl.BlockSpec(memory_space=pltpu.VMEM)] * 2,
        scratch_shapes=[
            pltpu.VMEM((OWNERS * ROWS, WIDTH), F32),
            pltpu.VMEM((BLOCKS, 2, 128), jnp.int32),
            pltpu.VMEM((BLOCKS, 2, 128), F32),
            pltpu.VMEM((BLOCKS, 6 * 256), BF16),
            pltpu.VMEM((8, BLOCKS), jnp.int32),
            pltpu.SMEM((8, BLOCKS), jnp.int32),
            pltpu.VMEM((8, CHUNK), jnp.int32),
            pltpu.SMEM((8, CHUNK), jnp.int32),
            pltpu.VMEM((CHUNK, WIDTH), F32),
            pltpu.SemaphoreType.DMA,
        ],
        compiler_params=pltpu.CompilerParams(vmem_limit_bytes=44 * 2**20),
        name="messages",
    )(table, meta, time, freq, weight, bias)


def update_kernel(memory, totals, counts, weight, bias, result, history, arrived, sems):
    t = lax.axis_index("tm")
    o = lax.axis_index("node")
    barrier = pltpu.get_barrier_semaphore()
    for k in range(1, PERIODS):
        pl.semaphore_signal(
            barrier, inc=1, device_id=(lax.rem(t + k, PERIODS), o), device_id_type=MESH
        )
    count = counts[...]
    count = jnp.concatenate([count, count], 1)
    mean = (totals[...] / jnp.maximum(count, 1.0)).astype(BF16)
    gates = dot(mean, weight[...])
    rate = jax.nn.sigmoid(gates[:, :WIDTH] + bias[...])
    candidate = jnp.tanh(gates[:, WIDTH:])
    touched = count > 0.0
    keep = jnp.where(touched, 1.0 - rate, 1.0)
    write = jnp.where(touched, rate * candidate, 0.0)
    mine = pl.ds(pl.multiple_of(t * SHARE, SHARE), SHARE)
    state = memory[mine, :]
    for k in range(PERIODS):
        rows = slice(k * SHARE, (k + 1) * SHARE)
        state = keep[rows] * state + write[rows]
        history[k] = state.astype(BF16)

        @pl.when(t == k)
        def _():
            result[mine, :] = state

    pl.semaphore_wait(barrier, PERIODS - 1)
    copies = []
    for k in range(1, PERIODS):
        to = lax.rem(t + k, PERIODS)
        copy = pltpu.make_async_remote_copy(
            src_ref=history.at[to],
            dst_ref=arrived.at[t],
            send_sem=sems.at[0, k],
            recv_sem=sems.at[1, k],
            device_id=(to, o),
            device_id_type=MESH,
        )
        copy.start()
        copies.append(copy)
    for k in (1, 7, 2, 6, 3, 5, 4):
        copies[k - 1].wait_recv()
        source = lax.rem(t + PERIODS - k, PERIODS)
        result[pl.ds(pl.multiple_of(source * SHARE, SHARE), SHARE), :] = arrived[source].astype(F32)
    for copy in copies:
        copy.wait_send()


def update(memory, totals, counts, weight, bias):
    return pl.pallas_call(
        update_kernel,
        out_shape=jax.ShapeDtypeStruct((ROWS, WIDTH), F32),
        in_specs=[pl.BlockSpec(memory_space=pltpu.VMEM)] * 5,
        out_specs=pl.BlockSpec(memory_space=pltpu.VMEM),
        scratch_shapes=[
            pltpu.VMEM((PERIODS, SHARE, WIDTH), BF16),
            pltpu.VMEM((PERIODS, SHARE, WIDTH), BF16),
            pltpu.SemaphoreType.DMA((2, PERIODS)),
        ],
        compiler_params=pltpu.CompilerParams(collective_id=1, has_side_effects=True),
        name="update",
    )(memory, totals, counts, weight, bias)


def shards(
    memory,
    src_slot,
    dst_slot,
    event_time,
    touched_rows,
    time_freq,
    msg_weight,
    msg_bias,
    gate_weight,
    update_bias,
):
    slots = jnp.concatenate([src_slot[0, 0], dst_slot[0, 0]])
    slots = jnp.broadcast_to(slots[:, None], (TERMS, 128))
    table, meta, time = spread(
        memory, slots, event_time[0], touched_rows.reshape(OWNERS, 1, 128)
    )
    totals, counts = messages(
        table.reshape(OWNERS * ROWS, WIDTH),
        meta.reshape(BLOCKS, 8, 128),
        time.reshape(BLOCKS, 8, 128),
        time_freq[None],
        msg_weight,
        msg_bias[None],
    )
    return update(memory, totals, counts, gate_weight, update_bias[None])[None]


def solution(mesh):
    return jax.shard_map(
        shards,
        mesh=mesh,
        in_specs=(
            P("node", None),
            P("tm", "node", None),
            P("tm", "node", None),
            P("tm", "node", None),
            P("tm", "node", None, None),
            P(),
            P(),
            P(),
            P(),
            P(),
        ),
        out_specs=P("tm", "node", None),
        check_vma=False,
    )
```

```python
import math

import jax
import jax.numpy as jnp
from jax import lax
from jax.experimental import pallas as pl
from jax.experimental.pallas import tpu as pltpu
from jax.sharding import PartitionSpec as P

MESH = pl.DeviceIdType.MESH
F32 = jnp.float32
BF16 = jnp.bfloat16
NT = (((1,), (1,)), ((), ()))
NN = (((1,), (0,)), ((), ()))

PERIODS = 8
OWNERS = 32
ROWS = 512
WIDTH = 256
TERMS = 1024
SHARE = ROWS // PERIODS
BLOCKS = PERIODS * OWNERS
CHUNK = 512
GROUP = 4
UNROLL = 32


def dot(a, b, dims=NN):
    return lax.dot_general(a, b, dims, preferred_element_type=F32)


def iota(shape, dim):
    return lax.broadcasted_iota(jnp.int32, shape, dim)


def where01(mask):
    return jnp.where(mask, 1.0, 0.0).astype(BF16)


def cosine(angle):
    turns = jnp.floor(angle * (0.5 / math.pi) + 0.5)
    rest = angle - turns * 6.28125
    rest = rest - turns * (2.0 * math.pi - 6.28125)
    square = rest * rest
    value = jnp.full_like(angle, 1.0 / math.factorial(16))
    for k in range(7, -1, -1):
        value = value * square + (-1.0) ** k / math.factorial(2 * k)
    return value


def sorted_terms(sources, targets, times, lists):
    lane = iota((TERMS, 128), 1)
    ones = jnp.ones((128, 128), BF16)
    square = iota((128, 128), 0) == iota((128, 128), 1)
    owners, places = [], []
    for slots in (sources, targets):
        for q in range(4):
            row = jnp.broadcast_to(slots[:, 128 * q : 128 * (q + 1)], (128, 128))
            owners.append(dot(jnp.where(square, row >> 7, 0).astype(F32).astype(BF16), ones))
            places.append(dot(jnp.where(square, row & 127, 0).astype(F32).astype(BF16), ones))
    owner = jnp.concatenate(owners, 0).astype(jnp.int32)
    slot = jnp.concatenate(places, 0).astype(jnp.int32)
    table = jnp.concatenate([(lists - 256).astype(F32), jnp.zeros((128 - OWNERS, 128), F32)], 0)
    per_owner = dot(where01(owner == lane), table.astype(BF16))
    picked = jnp.where(slot == lane, per_owner, 0.0).astype(BF16)
    row = dot(picked, ones).astype(jnp.int32) + 256
    node = owner * ROWS + row
    bucket = (node >> 6).astype(F32)
    rest = (node & 63).astype(F32)
    eighth = jnp.full((8, 128), 1.0 / 128.0, BF16)
    bucket_row = dot(eighth, bucket.astype(BF16), NT)
    rest_row = dot(eighth, rest.astype(BF16), NT)
    key_col = bucket * TERMS + iota((TERMS, 128), 0).astype(F32)
    key_row = bucket_row * TERMS + iota((8, TERMS), 1).astype(F32)
    below = jnp.zeros((TERMS, 128), F32)
    for q in range(8):
        part = jnp.broadcast_to(key_row[0:1, 128 * q : 128 * (q + 1)], (TERMS, 128))
        below = below + jnp.where(part < key_col, 1.0, 0.0)
    place = dot(below.astype(BF16), ones).astype(jnp.int32)
    half = TERMS // 2
    other_bucket = jnp.concatenate([bucket_row[:, half:], bucket_row[:, :half]], 1)
    other_rest = jnp.concatenate([rest_row[:, half:], rest_row[:, :half]], 1)
    time = jnp.broadcast_to(jnp.concatenate([times, times], 1), (8, TERMS))
    t1 = time.astype(BF16).astype(F32)
    t2 = (time - t1).astype(BF16).astype(F32)
    t3 = time - t1 - t2
    which = iota((8, TERMS), 0)
    meta = jnp.zeros((8, TERMS), F32)
    for k, piece in enumerate((bucket_row, rest_row, other_bucket, other_rest, t1, t2, t3)):
        meta = jnp.where(which == k, piece, meta)
    meta = meta.astype(BF16)
    rows = []
    for q in range(8):
        out = dot(meta, where01(place == lane + 128 * q))
        whole = out.astype(jnp.int32)
        own = whole[0:1] * 64 + whole[1:2]
        other = whole[2:3] * 64 + whole[3:4]
        rows.append(((own << 14) | other, out[4:5] + out[5:6] + out[6:7]))
    return rows


class Gather:
    OPS = 36
    COLUMNS = ((0, 0), (1, -1), (2, 1), (3, 2))
    PLACES = (0, -1, 1, 2)

    def __init__(self, ref, start, size, first, base, sems, at, landed=None):
        self.ref = ref
        self.full = (pl.ds(start, size),)
        self.top = (pl.ds(start, size // 2),)
        self.bottom = (pl.ds(start + size // 2, size // 2),)
        self.first, self.base, self.sems, self.at = first, base, sems, at
        self.landed = landed
        self.started = {}

    def node(self, du, dv, flip=False):
        t, x, y, c = self.at
        dx, dy = (du, dv) if self.first == 0 else (dv, du)
        core = 1 - c if flip else c
        return (lax.rem(x + dx + 4, 4) * 4 + lax.rem(y + dy + 4, 4)) * 2 + core

    def land(self, du, dv, flip=False):
        if self.landed is not None:
            self.landed(self.node(du, dv, flip), self.full)

    def start(self, op, du, dv, part, to):
        piece = self.ref.at[(self.node(du, dv),) + part]
        copy = pltpu.make_async_remote_copy(
            src_ref=piece,
            dst_ref=piece,
            send_sem=self.sems.at[0, self.base + op],
            recv_sem=self.sems.at[1, self.base + op],
            device_id=(self.at[0], to),
            device_id_type=MESH,
        )
        copy.start()
        self.started[op] = copy

    def wait(self, op):
        self.started[op].wait_recv()

    def share(self, k, du, dv):
        self.start(20 + k, du, dv, self.full, self.node(0, 0, True))

    def second(self, i, du):
        self.start(4 + 4 * i, du, 0, self.full, self.node(0, 1))
        self.start(5 + 4 * i, du, 0, self.full, self.node(0, -1))
        self.share(4 * i, du, 0)

    def begin(self):
        self.start(0, 0, 0, self.full, self.node(1, 0))
        self.start(1, 0, 0, self.full, self.node(-1, 0))

    def own_second(self):
        self.second(0, 0)

    def near(self):
        self.wait(0)
        self.start(2, -1, 0, self.top, self.node(1, 0))
        self.second(1, -1)
        self.wait(1)
        self.start(3, 1, 0, self.bottom, self.node(-1, 0))
        self.second(2, 1)
        self.land(-1, 0)
        self.land(1, 0)

    def far(self):
        self.wait(2)
        self.wait(3)
        self.second(3, 2)
        self.land(2, 0)

    def column_near(self, i):
        du = self.PLACES[i]
        self.wait(4 + 4 * i)
        self.start(6 + 4 * i, du, -1, self.top, self.node(0, 1))
        self.share(4 * i + 1, du, -1)
        self.wait(5 + 4 * i)
        self.start(7 + 4 * i, du, 1, self.bottom, self.node(0, -1))
        self.share(4 * i + 2, du, 1)
        self.land(du, -1)
        self.land(du, 1)

    def column_far(self, i):
        du = self.PLACES[i]
        self.wait(6 + 4 * i)
        self.wait(7 + 4 * i)
        self.share(4 * i + 3, du, 2)
        self.land(du, 2)

    def shared(self, *ks):
        for k in ks:
            self.wait(20 + k)
            self.land(self.PLACES[k // 4], self.PLACES[k % 4], True)

    def finish(self):
        for copy in self.started.values():
            copy.wait_send()


def spread_kernel(
    memory_h, source_h, target_h, moment_h, lists_h, wide, meta, time,
    memory, source, target, moment, lists, table, block_lists, load_sems, sems, list_sems, share_sems,
):
    t = lax.axis_index("tm")
    o = lax.axis_index("node")
    x, y, c = o // 8, lax.rem(o // 2, 4), lax.rem(o, 2)
    at = (t, x, y, c)
    loads = [
        pltpu.make_async_copy(src, dst, load_sems.at[i])
        for i, (src, dst) in enumerate(
            (
                (memory_h, memory),
                (lists_h, lists),
                (source_h, source),
                (target_h, target),
                (moment_h, moment),
            )
        )
    ]
    for load in loads:
        load.start()
    barrier = pltpu.get_barrier_semaphore()

    def greet(k, carry):
        pl.semaphore_signal(
            barrier, inc=1, device_id=(t, lax.rem(o + k, OWNERS)), device_id_type=MESH
        )
        return carry

    def greet_periods(k, carry):
        pl.semaphore_signal(
            barrier, inc=1, device_id=(lax.rem(t + k, PERIODS), o), device_id_type=MESH
        )
        return carry

    lax.fori_loop(1, OWNERS, greet, 0)
    lax.fori_loop(1, PERIODS, greet_periods, 0)
    for load in loads:
        load.wait()
    table[pl.ds(o, 1)] = memory[...].astype(BF16)[None]
    block_lists[pl.ds(o, 1)] = lists[pl.ds(o, 1)]

    def widen(node, part):
        rows = part[0]
        wide[pl.ds(pl.multiple_of(node * ROWS + rows.start, 64), rows.size), :] = table[
            node, rows, :
        ].astype(F32)

    pl.semaphore_wait(barrier, OWNERS - 1 + PERIODS - 1)

    def list_copy(k):
        to = lax.rem(o + k, OWNERS)
        return pltpu.make_async_remote_copy(
            src_ref=lists.at[to],
            dst_ref=block_lists.at[o],
            send_sem=list_sems.at[0, k],
            recv_sem=list_sems.at[1, k],
            device_id=(t, to),
            device_id_type=MESH,
        )

    def wait_list(k, carry):
        list_copy(k).wait()
        return carry

    for k in FAR_FIRST:
        for core in range(2):
            if k + core:
                list_copy(2 * k + core).start()
    n = Gather.OPS
    big = (
        Gather(table, 0, 256, 0, 0, sems, at, widen),
        Gather(table, 256, 256, 1, n, sems, at, widen),
    )
    chip = o // 2
    pair = (meta, time)

    def list_send(j, piece, to, op):
        copy = pltpu.make_async_remote_copy(
            src_ref=piece,
            dst_ref=piece,
            send_sem=share_sems.at[0, j, op],
            recv_sem=share_sems.at[1, j, op],
            device_id=to,
            device_id_type=MESH,
        )
        copy.start()
        sent[j, op] = copy

    sent = {}

    def plane_send():
        for k in FAR_FIRST[:-1]:
            to = lax.rem(chip + k, 16) * 2 + c
            for j in range(2):
                list_send(j, pair[j].at[c, t, chip], (t, to), k)

    def plane_take():
        for k in range(1, 16):
            for j in range(2):
                sent[j, k].wait_recv()

    def period(step):
        return lax.rem(t + step + PERIODS, PERIODS)

    def ring_start(step):
        whole = step < 3
        for j in range(2):
            if step:
                sent[j, 16 + 2 * (step - 1)].wait_recv()
            up = pair[j].at[c, period(-step)]
            list_send(j, up if whole else up.at[pl.ds(0, 8)], (period(1), o), 16 + 2 * step)
            if step:
                sent[j, 17 + 2 * (step - 1)].wait_recv()
            down = pair[j].at[c, period(step)]
            list_send(j, down if whole else down.at[pl.ds(8, 8)], (period(-1), o), 17 + 2 * step)

    def ring_end():
        for j in range(2):
            sent[j, 22].wait_recv()
            sent[j, 23].wait_recv()

    def partner_send(*steps):
        for step in steps:
            for j in range(2):
                list_send(j, pair[j].at[c, period(step)], (t, o + 1 - 2 * c), 24 + step % 8)

    def partner_take():
        for step in range(8):
            for j in range(2):
                sent[j, 24 + step].wait_recv()

    def own_rows():
        for start in (0, 256):
            widen(o, (pl.ds(start, 256),))

    def sort():
        lax.fori_loop(1, OWNERS, wait_list, 0)
        rows = sorted_terms(source[...], target[...], moment[...], block_lists[:, 0, :])
        for q, (meta_row, time_row) in enumerate(rows):
            meta[c, t, chip, pl.ds(q, 1), :] = meta_row
            time[c, t, chip, pl.ds(q, 1), :] = time_row

    def both(group, step, *numbers):
        for g in group:
            getattr(g, step)(*numbers)

    def run(order):
        for word in order:
            if word == "own":
                own_rows()
            elif word == "sort":
                sort()
            elif word == "plane":
                plane_send()
            elif word == "taken":
                plane_take()
            elif word == "end":
                ring_end()
            elif word == "partner":
                partner_take()
            elif word[0] == "R":
                ring_start(int(word[1]))
            elif word[0] == "P":
                partner_send(*(int(k) for k in word[1:].split(",")))
            else:
                numbers = [int(k) for k in word[2:].split(",") if k]
                step = STEPS[word[1]]
                if step == "shared" or not numbers:
                    both(big, step, *numbers)
                else:
                    for k in numbers:
                        both(big, step, k)

    run(ORDER)
    for g in big:
        g.finish()
    for copy in sent.values():
        copy.wait_send()


FAR_FIRST = (10, 6, 9, 11, 14, 2, 5, 7, 8, 13, 15, 1, 3, 4, 12, 0)
STEPS = {
    "b": "begin",
    "s": "own_second",
    "n": "near",
    "f": "far",
    "c": "column_near",
    "d": "column_far",
    "h": "shared",
}
ORDER = (
    "Mb", "Ms", "own", "sort", "plane", "Mn", "taken", "R0", "P0", "Mf", "Mc0", "R1",
    "P1,-1", "Mc1", "Mh0,4,8", "R2", "P2,-2", "Mc2", "Mh1,2,12", "R3", "P3,-3", "Mc3",
    "Md0", "Mh5,6", "Md1", "Mh9,10", "end", "P4", "Md2", "Mh13,14", "Md3", "Mh3,7,11,15",
    "partner",
)

VMEM = pl.BlockSpec(memory_space=pltpu.VMEM)
HBM = pl.BlockSpec(memory_space=pltpu.HBM)


def in_hbm(*arrays):
    return [pltpu.with_memory_space_constraint(a, pltpu.HBM) for a in arrays]


def spread(*arrays):
    return pl.pallas_call(
        spread_kernel,
        out_shape=(
            jax.ShapeDtypeStruct((OWNERS * ROWS, WIDTH), F32),
            jax.ShapeDtypeStruct((2, PERIODS, OWNERS // 2, 8, 128), jnp.int32),
            jax.ShapeDtypeStruct((2, PERIODS, OWNERS // 2, 8, 128), F32),
        ),
        in_specs=[HBM] * 5,
        out_specs=[VMEM] * 3,
        scratch_shapes=[
            pltpu.VMEM((ROWS, WIDTH), F32),
            pltpu.VMEM((1, ROWS), jnp.int32),
            pltpu.VMEM((1, ROWS), jnp.int32),
            pltpu.VMEM((1, ROWS), F32),
            pltpu.VMEM((OWNERS, 1, 128), jnp.int32),
            pltpu.VMEM((OWNERS, ROWS, WIDTH), BF16),
            pltpu.VMEM((OWNERS, 1, 128), jnp.int32),
            pltpu.SemaphoreType.DMA((5,)),
            pltpu.SemaphoreType.DMA((2, 2 * Gather.OPS)),
            pltpu.SemaphoreType.DMA((2, OWNERS)),
            pltpu.SemaphoreType.DMA((2, 2, 32)),
        ],
        compiler_params=pltpu.CompilerParams(
            collective_id=0, has_side_effects=True, vmem_limit_bytes=28 * 2**20
        ),
        name="spread",
    )(*in_hbm(*arrays))


def message_kernel(
    wide, meta, time, freq_h, weight_h, bias_h, memory_h, totals, counts,
    freq, weight, bias, memory, windows, window_times, pieces, rows_v, rows_s, index_v, index_s,
    segments, parts, gathered, sem, index_sems, load_sems,
):
    t = lax.axis_index("tm")
    bucket = lax.axis_index("node") * PERIODS + t
    mine = pl.ds(pl.multiple_of(t * SHARE, SHARE), SHARE)
    loads = [
        pltpu.make_async_copy(src, dst, load_sems.at[i])
        for i, (src, dst) in enumerate(
            ((freq_h, freq), (weight_h, weight), (bias_h, bias), (memory_h.at[mine], memory))
        )
    ]
    for load in loads:
        load.start()
    totals[...] = jnp.zeros_like(totals)
    counts[...] = jnp.zeros_like(counts)
    gathered[...] = jnp.zeros_like(gathered)
    start_parts, end_parts = [], []
    for i in range(8):
        own = meta[pl.ds(32 * i, 32)] >> 20
        start_parts.append(jnp.sum(jnp.where(own < bucket, 1.0, 0.0), axis=1))
        end_parts.append(jnp.sum(jnp.where(own <= bucket, 1.0, 0.0), axis=1))
    ones_row = jnp.ones((8, 128), BF16)
    start = dot(ones_row, jnp.concatenate(start_parts, 0).astype(BF16), NT)
    end = dot(ones_row, jnp.concatenate(end_parts, 0).astype(BF16), NT)
    upper = where01(iota((BLOCKS, BLOCKS), 0) < iota((BLOCKS, BLOCKS), 1))
    ones_wide = jnp.ones((8, BLOCKS), BF16)
    ones_col = jnp.ones((BLOCKS, 128), BF16)
    ones_term = jnp.ones((CHUNK, 128), BF16)
    longest = jnp.max(end - start)
    for load in loads:
        load.wait()
    own_rows = memory[...].astype(BF16)
    own_rows = jnp.concatenate([own_rows, jnp.zeros((128 - SHARE, WIDTH), BF16)], 0)
    freqs = jnp.broadcast_to(freq[...], (CHUNK, 128))

    def index_copy(ch):
        return pltpu.make_async_copy(index_v.at[ch], index_s.at[ch], index_sems.at[ch])

    def one_round(r, carry):
        begin = start + (r * 128).astype(F32)
        size = jnp.clip(end - begin, 0.0, 128.0)
        before = dot(size.astype(BF16), upper)
        which = iota((8, BLOCKS), 0)
        begin_i = begin.astype(jnp.int32)
        rows_v[...] = jnp.where(which == 0, begin_i, (before + size).astype(jnp.int32))
        copy = pltpu.make_async_copy(rows_v, rows_s, sem)
        copy.start()
        copy.wait()
        total = rows_s[1, BLOCKS - 1]

        def fetch(i, carry):
            for u in range(8):
                b = i * 8 + u
                at = rows_s[0, b] >> 7
                for j in range(2):
                    from_row = pl.ds(jnp.minimum(at + j, 7), 1)
                    windows[j, pl.ds(b, 1), :] = meta[b, from_row, :]
                    window_times[j, pl.ds(b, 1), :] = time[b, from_row, :]
            return carry

        lax.fori_loop(0, BLOCKS // 8, fetch, 0)
        for j in range(2):
            m = windows[j]
            w = window_times[j]
            period = (iota((BLOCKS, 128), 0) >> 4) & 7
            seg = period * SHARE + ((m >> 14) & 63) - 256
            t1 = w.astype(BF16).astype(F32)
            t2 = (w - t1).astype(BF16).astype(F32)
            t3 = w - t1 - t2
            for k, piece in enumerate(
                (seg.astype(F32), ((m >> 6) & 255).astype(F32), (m & 63).astype(F32), t1, t2, t3)
            ):
                pieces[:, 256 * k + 128 * j : 256 * k + 128 * (j + 1)] = piece.astype(BF16)
        offset = (begin_i & 127).astype(F32) - before

        def one_group(group, carry):
            first = group * GROUP * CHUNK

            def locate(ch, carry):
                at = first + ch * CHUNK
                p = (at + iota((CHUNK, BLOCKS), 0)).astype(F32)
                low = jnp.broadcast_to(before[0:1], (CHUNK, BLOCKS))
                high = low + jnp.broadcast_to(size[0:1], (CHUNK, BLOCKS))
                hit = (low <= p) & (p < high)
                shift = jnp.sum(
                    jnp.where(hit, jnp.broadcast_to(offset[0:1], (CHUNK, BLOCKS)), 0.0),
                    axis=1,
                    keepdims=True,
                )
                found = dot(where01(hit), pieces[...])
                here = (p + shift) == iota((CHUNK, BLOCKS), 1).astype(F32)
                chosen = [
                    jnp.where(here, found[:, 256 * k : 256 * (k + 1)], 0.0).astype(BF16)
                    for k in range(6)
                ]
                other = dot(ones_wide, chosen[1], NT) * 64.0 + dot(ones_wide, chosen[2], NT)
                index_v[ch] = other.astype(jnp.int32)
                index_copy(ch).start()
                seg_row = dot(ones_wide, chosen[0], NT) + 256.0
                lane_p = at + iota((8, CHUNK), 1)
                segments[ch] = jnp.where(lane_p < total, seg_row, -1.0)
                seg_col = dot(chosen[0], ones_col).astype(jnp.int32) + 256
                own_hot = where01((seg_col & 63) == iota((CHUNK, 128), 1))
                own = dot(own_hot, own_rows).astype(BF16)
                moment = (
                    dot(chosen[3], ones_col) + dot(chosen[4], ones_col) + dot(chosen[5], ones_col)
                )
                encoding = cosine(moment * freqs).astype(BF16)
                parts[ch] = dot(own, weight[pl.ds(0, WIDTH), :]) + dot(
                    encoding, weight[pl.ds(2 * WIDTH, 128), :]
                )
                parts[ch] = parts[ch] + bias[...]
                return carry

            def collect(ch, carry):
                index_copy(ch).wait()

                def pick(i, carry):
                    for u in range(UNROLL):
                        q = i * UNROLL + u
                        gathered[pl.ds(q, 1), :] = wide[pl.ds(index_s[ch, 0, q], 1), :]
                    return carry

                left = jnp.minimum(total - first - ch * CHUNK, CHUNK)
                lax.fori_loop(0, (left + UNROLL - 1) // UNROLL, pick, 0)
                other = dot(gathered[...].astype(BF16), weight[pl.ds(WIDTH, WIDTH), :])
                message = jnp.maximum(parts[ch] + other, 0.0)
                seg_hot = where01(
                    iota((ROWS, CHUNK), 0).astype(F32)
                    == jnp.broadcast_to(segments[ch, 0:1, :], (ROWS, CHUNK))
                )
                upper_part = message.astype(BF16)
                lower_part = (message - upper_part.astype(F32)).astype(BF16)
                totals[...] += dot(seg_hot, upper_part) + dot(seg_hot, lower_part)
                counts[...] += dot(seg_hot, ones_term)
                return carry

            chunks = jnp.minimum((total - first + CHUNK - 1) // CHUNK, GROUP)
            lax.fori_loop(0, chunks, locate, 0)
            lax.fori_loop(0, chunks, collect, 0)
            return carry

        lax.fori_loop(0, (total + GROUP * CHUNK - 1) // (GROUP * CHUNK), one_group, 0)
        return carry

    rounds = (longest.astype(jnp.int32) + 127) // 128
    lax.fori_loop(0, rounds, one_round, 0)


def messages(wide, meta, time, *others):
    return pl.pallas_call(
        message_kernel,
        out_shape=(
            jax.ShapeDtypeStruct((ROWS, WIDTH), F32),
            jax.ShapeDtypeStruct((ROWS, 128), F32),
        ),
        in_specs=[VMEM] * 3 + [HBM] * 4,
        out_specs=[VMEM] * 2,
        scratch_shapes=[
            pltpu.VMEM((1, 128), F32),
            pltpu.VMEM((2 * WIDTH + 128, WIDTH), BF16),
            pltpu.VMEM((1, WIDTH), F32),
            pltpu.VMEM((SHARE, WIDTH), F32),
            pltpu.VMEM((2, BLOCKS, 128), jnp.int32),
            pltpu.VMEM((2, BLOCKS, 128), F32),
            pltpu.VMEM((BLOCKS, 6 * 256), BF16),
            pltpu.VMEM((8, BLOCKS), jnp.int32),
            pltpu.SMEM((8, BLOCKS), jnp.int32),
            pltpu.VMEM((GROUP, 8, CHUNK), jnp.int32),
            pltpu.SMEM((GROUP, 8, CHUNK), jnp.int32),
            pltpu.VMEM((GROUP, 8, CHUNK), F32),
            pltpu.VMEM((GROUP, CHUNK, WIDTH), F32),
            pltpu.VMEM((CHUNK, WIDTH), F32),
            pltpu.SemaphoreType.DMA,
            pltpu.SemaphoreType.DMA((GROUP,)),
            pltpu.SemaphoreType.DMA((4,)),
        ],
        compiler_params=pltpu.CompilerParams(vmem_limit_bytes=16 * 2**20),
        name="messages",
    )(wide, meta, time, *in_hbm(*others))


def update_kernel(
    totals, counts, memory_h, weight_h, bias_h, arrived, final, memory, weight, bias, history,
    load_sems, sems,
):
    t = lax.axis_index("tm")
    o = lax.axis_index("node")
    mine = pl.ds(pl.multiple_of(t * SHARE, SHARE), SHARE)
    loads = [
        pltpu.make_async_copy(src, dst, load_sems.at[i])
        for i, (src, dst) in enumerate(
            ((memory_h.at[mine], memory), (weight_h, weight), (bias_h, bias))
        )
    ]
    for load in loads:
        load.start()
    barrier = pltpu.get_barrier_semaphore()
    for k in range(1, PERIODS):
        pl.semaphore_signal(
            barrier, inc=1, device_id=(lax.rem(t + k, PERIODS), o), device_id_type=MESH
        )
    count = counts[...]
    count = jnp.concatenate([count, count], 1)
    mean = (totals[...] / jnp.maximum(count, 1.0)).astype(BF16)
    for load in loads:
        load.wait()
    gates = dot(mean, weight[...])
    rate = jax.nn.sigmoid(gates[:, :WIDTH] + bias[...])
    candidate = jnp.tanh(gates[:, WIDTH:])
    touched = count > 0.0
    keep = jnp.where(touched, 1.0 - rate, 1.0)
    write = jnp.where(touched, rate * candidate, 0.0)
    state = memory[...]
    for k in range(PERIODS):
        rows = slice(k * SHARE, (k + 1) * SHARE)
        state = keep[rows] * state + write[rows]
        history[k] = state.astype(BF16)

        @pl.when(t == k)
        def _():
            final[...] = state

    pl.semaphore_wait(barrier, PERIODS - 1)
    copies = []
    for k in (4, 3, 5, 2, 6, 1, 7):
        to = lax.rem(t + k, PERIODS)
        copy = pltpu.make_async_remote_copy(
            src_ref=history.at[to],
            dst_ref=arrived.at[t],
            send_sem=sems.at[0, k],
            recv_sem=sems.at[1, k],
            device_id=(to, o),
            device_id_type=MESH,
        )
        copy.start()
        copies.append(copy)
    arrived[pl.ds(t, 1)] = history[pl.ds(t, 1)]
    for copy in copies:
        copy.wait()


def update(totals, counts, memory, weight, bias):
    return pl.pallas_call(
        update_kernel,
        out_shape=(
            jax.ShapeDtypeStruct((PERIODS, SHARE, WIDTH), BF16),
            jax.ShapeDtypeStruct((SHARE, WIDTH), F32),
        ),
        in_specs=[VMEM] * 2 + [HBM] * 3,
        out_specs=[VMEM] * 2,
        scratch_shapes=[
            pltpu.VMEM((SHARE, WIDTH), F32),
            pltpu.VMEM((WIDTH, 2 * WIDTH), BF16),
            pltpu.VMEM((1, WIDTH), F32),
            pltpu.VMEM((PERIODS, SHARE, WIDTH), BF16),
            pltpu.SemaphoreType.DMA((3,)),
            pltpu.SemaphoreType.DMA((2, PERIODS)),
        ],
        compiler_params=pltpu.CompilerParams(
            collective_id=1, has_side_effects=True, vmem_limit_bytes=16 * 2**20
        ),
        name="update",
    )(totals, counts, *in_hbm(memory, weight, bias))


def shards(
    memory,
    src_slot,
    dst_slot,
    event_time,
    touched_rows,
    time_freq,
    msg_weight,
    msg_bias,
    gate_weight,
    update_bias,
):
    wide, meta, time = spread(
        memory,
        src_slot[0],
        dst_slot[0],
        event_time[0],
        touched_rows.reshape(OWNERS, 1, 128),
    )
    totals, counts = messages(
        wide,
        meta.reshape(BLOCKS, 8, 128),
        time.reshape(BLOCKS, 8, 128),
        time_freq[None],
        msg_weight,
        msg_bias[None],
        memory,
    )
    arrived, final = update(totals, counts, memory, gate_weight, update_bias[None])
    mine = lax.broadcasted_iota(jnp.int32, (PERIODS, SHARE, WIDTH), 0) == lax.axis_index("tm")
    result = jnp.where(mine, final[None], arrived.astype(F32))
    return result.reshape(1, ROWS, WIDTH)


def solution(mesh):
    return jax.shard_map(
        shards,
        mesh=mesh,
        in_specs=(
            P("node", None),
            P("tm", "node", None),
            P("tm", "node", None),
            P("tm", "node", None),
            P("tm", "node", None, None),
            P(),
            P(),
            P(),
            P(),
            P(),
        ),
        out_specs=P("tm", "node", None),
        check_vma=False,
    )
```

```python
import math

import jax
import jax.numpy as jnp
from jax import lax
from jax.experimental import pallas as pl
from jax.experimental.pallas import tpu as pltpu
from jax.sharding import PartitionSpec as P

MESH = pl.DeviceIdType.MESH
F32 = jnp.float32
BF16 = jnp.bfloat16
NT = (((1,), (1,)), ((), ()))
NN = (((1,), (0,)), ((), ()))

PERIODS = 8
OWNERS = 32
ROWS = 512
WIDTH = 256
TERMS = 1024
SHARE = ROWS // PERIODS
BLOCKS = PERIODS * OWNERS
CHUNK = 512
GROUP = 4
UNROLL = 32


def dot(a, b, dims=NN):
    return lax.dot_general(a, b, dims, preferred_element_type=F32)


def iota(shape, dim):
    return lax.broadcasted_iota(jnp.int32, shape, dim)


def where01(mask):
    return jnp.where(mask, 1.0, 0.0).astype(BF16)


def cosine(angle):
    turns = jnp.floor(angle * (0.5 / math.pi) + 0.5)
    rest = angle - turns * 6.28125
    rest = rest - turns * (2.0 * math.pi - 6.28125)
    square = rest * rest
    value = jnp.full_like(angle, 1.0 / math.factorial(16))
    for k in range(7, -1, -1):
        value = value * square + (-1.0) ** k / math.factorial(2 * k)
    return value


def sorted_terms(sources, targets, times, lists):
    lane = iota((TERMS, 128), 1)
    ones = jnp.ones((128, 128), BF16)
    square = iota((128, 128), 0) == iota((128, 128), 1)
    owners, places = [], []
    for slots in (sources, targets):
        for q in range(4):
            row = jnp.broadcast_to(slots[:, 128 * q : 128 * (q + 1)], (128, 128))
            owners.append(dot(jnp.where(square, row >> 7, 0).astype(F32).astype(BF16), ones))
            places.append(dot(jnp.where(square, row & 127, 0).astype(F32).astype(BF16), ones))
    owner = jnp.concatenate(owners, 0).astype(jnp.int32)
    slot = jnp.concatenate(places, 0).astype(jnp.int32)
    table = jnp.concatenate([(lists - 256).astype(F32), jnp.zeros((128 - OWNERS, 128), F32)], 0)
    per_owner = dot(where01(owner == lane), table.astype(BF16))
    picked = jnp.where(slot == lane, per_owner, 0.0).astype(BF16)
    row = dot(picked, ones).astype(jnp.int32) + 256
    node = owner * ROWS + row
    bucket = (node >> 6).astype(F32)
    rest = (node & 63).astype(F32)
    eighth = jnp.full((8, 128), 1.0 / 128.0, BF16)
    bucket_row = dot(eighth, bucket.astype(BF16), NT)
    rest_row = dot(eighth, rest.astype(BF16), NT)
    key_col = bucket * TERMS + iota((TERMS, 128), 0).astype(F32)
    key_row = bucket_row * TERMS + iota((8, TERMS), 1).astype(F32)
    below = jnp.zeros((TERMS, 128), F32)
    for q in range(8):
        part = jnp.broadcast_to(key_row[0:1, 128 * q : 128 * (q + 1)], (TERMS, 128))
        below = below + jnp.where(part < key_col, 1.0, 0.0)
    place = dot(below.astype(BF16), ones).astype(jnp.int32)
    half = TERMS // 2
    other_bucket = jnp.concatenate([bucket_row[:, half:], bucket_row[:, :half]], 1)
    other_rest = jnp.concatenate([rest_row[:, half:], rest_row[:, :half]], 1)
    time = jnp.broadcast_to(jnp.concatenate([times, times], 1), (8, TERMS))
    t1 = time.astype(BF16).astype(F32)
    t2 = (time - t1).astype(BF16).astype(F32)
    t3 = time - t1 - t2
    which = iota((8, TERMS), 0)
    meta = jnp.zeros((8, TERMS), F32)
    for k, piece in enumerate((bucket_row, rest_row, other_bucket, other_rest, t1, t2, t3)):
        meta = jnp.where(which == k, piece, meta)
    meta = meta.astype(BF16)
    rows = []
    for q in range(8):
        out = dot(meta, where01(place == lane + 128 * q))
        whole = out.astype(jnp.int32)
        own = whole[0:1] * 64 + whole[1:2]
        other = whole[2:3] * 64 + whole[3:4]
        rows.append(((own << 14) | other, out[4:5] + out[5:6] + out[6:7]))
    return rows


class Gather:
    OPS = 36
    COLUMNS = ((0, 0), (1, -1), (2, 1), (3, 2))
    PLACES = (0, -1, 1, 2)

    def __init__(self, ref, start, size, first, base, sems, at, landed=None):
        self.ref = ref
        self.full = (pl.ds(start, size),)
        self.top = (pl.ds(start, size // 2),)
        self.bottom = (pl.ds(start + size // 2, size // 2),)
        self.first, self.base, self.sems, self.at = first, base, sems, at
        self.landed = landed
        self.started = {}

    def node(self, du, dv, flip=False):
        t, x, y, c = self.at
        dx, dy = (du, dv) if self.first == 0 else (dv, du)
        core = 1 - c if flip else c
        return (lax.rem(x + dx + 4, 4) * 4 + lax.rem(y + dy + 4, 4)) * 2 + core

    def land(self, du, dv, flip=False):
        if self.landed is not None:
            self.landed(self.node(du, dv, flip), self.full)

    def start(self, op, du, dv, part, to):
        piece = self.ref.at[(self.node(du, dv),) + part]
        copy = pltpu.make_async_remote_copy(
            src_ref=piece,
            dst_ref=piece,
            send_sem=self.sems.at[0, self.base + op],
            recv_sem=self.sems.at[1, self.base + op],
            device_id=(self.at[0], to),
            device_id_type=MESH,
        )
        copy.start()
        self.started[op] = copy

    def wait(self, op):
        self.started[op].wait_recv()

    def share(self, k, du, dv):
        self.start(20 + k, du, dv, self.full, self.node(0, 0, True))

    def second(self, i, du):
        self.start(4 + 4 * i, du, 0, self.full, self.node(0, 1))
        self.start(5 + 4 * i, du, 0, self.full, self.node(0, -1))
        self.share(4 * i, du, 0)

    def begin(self):
        self.start(0, 0, 0, self.full, self.node(1, 0))
        self.start(1, 0, 0, self.full, self.node(-1, 0))

    def own_second(self):
        self.second(0, 0)

    def near(self):
        self.wait(0)
        self.start(2, -1, 0, self.top, self.node(1, 0))
        self.wait(1)
        self.start(3, 1, 0, self.bottom, self.node(-1, 0))
        self.second(1, -1)

    def near_second(self):
        self.second(2, 1)
        self.land(-1, 0)
        self.land(1, 0)

    def far(self):
        self.wait(2)
        self.wait(3)
        self.second(3, 2)
        self.land(2, 0)

    def column_near(self, i):
        du = self.PLACES[i]
        self.wait(4 + 4 * i)
        self.start(6 + 4 * i, du, -1, self.top, self.node(0, 1))
        self.share(4 * i + 1, du, -1)
        self.wait(5 + 4 * i)
        self.start(7 + 4 * i, du, 1, self.bottom, self.node(0, -1))
        self.share(4 * i + 2, du, 1)
        self.land(du, -1)
        self.land(du, 1)

    def column_far(self, i):
        du = self.PLACES[i]
        self.wait(6 + 4 * i)
        self.wait(7 + 4 * i)
        self.share(4 * i + 3, du, 2)
        self.land(du, 2)

    def shared(self, *ks):
        for k in ks:
            self.wait(20 + k)
            self.land(self.PLACES[k // 4], self.PLACES[k % 4], True)

    def finish(self):
        for copy in self.started.values():
            copy.wait_send()


def spread_kernel(
    memory_h, source_h, target_h, moment_h, lists_h, wide, meta, time,
    memory, source, target, moment, lists, table, block_lists, load_sems, sems, list_sems, share_sems,
):
    t = lax.axis_index("tm")
    o = lax.axis_index("node")
    x, y, c = o // 8, lax.rem(o // 2, 4), lax.rem(o, 2)
    at = (t, x, y, c)
    loads = [
        pltpu.make_async_copy(src, dst, load_sems.at[i])
        for i, (src, dst) in enumerate(
            (
                (memory_h, memory),
                (lists_h, lists),
                (source_h, source),
                (target_h, target),
                (moment_h, moment),
            )
        )
    ]
    for load in loads:
        load.start()
    barrier = pltpu.get_barrier_semaphore()

    def greet(k, carry):
        pl.semaphore_signal(
            barrier, inc=1, device_id=(t, lax.rem(o + k, OWNERS)), device_id_type=MESH
        )
        return carry

    def greet_periods(k, carry):
        pl.semaphore_signal(
            barrier, inc=1, device_id=(lax.rem(t + k, PERIODS), o), device_id_type=MESH
        )
        return carry

    lax.fori_loop(1, OWNERS, greet, 0)
    lax.fori_loop(1, PERIODS, greet_periods, 0)
    for load in loads:
        load.wait()
    table[pl.ds(o, 1)] = memory[...].astype(BF16)[None]
    block_lists[pl.ds(o, 1)] = lists[pl.ds(o, 1)]

    def widen(node, part):
        rows = part[0]
        piece = table[node, rows, :].astype(F32)
        first = pl.multiple_of((node * ROWS + rows.start) * 2, 128)
        for side in range(2):
            wide[pl.ds(first + side, rows.size, stride=2), :] = piece[:, 128 * side : 128 * side + 128]

    pl.semaphore_wait(barrier, OWNERS - 1 + PERIODS - 1)

    def list_copy(k):
        to = lax.rem(o + k, OWNERS)
        return pltpu.make_async_remote_copy(
            src_ref=lists.at[to],
            dst_ref=block_lists.at[o],
            send_sem=list_sems.at[0, k],
            recv_sem=list_sems.at[1, k],
            device_id=(t, to),
            device_id_type=MESH,
        )

    def wait_list(k, carry):
        list_copy(k).wait()
        return carry

    for k in FAR_FIRST:
        for core in range(2):
            if k + core:
                list_copy(2 * k + core).start()
    n = Gather.OPS
    big = (
        Gather(table, 0, 256, 0, 0, sems, at, widen),
        Gather(table, 256, 256, 1, n, sems, at, widen),
    )
    chip = o // 2
    pair = (meta, time)

    def list_send(j, piece, to, op):
        copy = pltpu.make_async_remote_copy(
            src_ref=piece,
            dst_ref=piece,
            send_sem=share_sems.at[0, j, op],
            recv_sem=share_sems.at[1, j, op],
            device_id=to,
            device_id_type=MESH,
        )
        copy.start()
        sent[j, op] = copy

    sent = {}

    def plane_send():
        for k in FAR_FIRST[:-1]:
            to = lax.rem(chip + k, 16) * 2 + c
            for j in range(2):
                list_send(j, pair[j].at[c, t, chip], (t, to), k)

    def plane_take():
        for k in range(1, 16):
            for j in range(2):
                sent[j, k].wait_recv()

    def period(step):
        return lax.rem(t + step + PERIODS, PERIODS)

    def ring_op(step, half, side):
        return 16 + 4 * step + 2 * half + side

    def ring_start(step):
        for j in range(2):
            for half in range(2):
                for side in range(2):
                    if step:
                        sent[j, ring_op(step - 1, half, side)].wait_recv()
                    if step < 3 or half == side:
                        piece = pair[j].at[c, period(step if side else -step), pl.ds(8 * half, 8)]
                        to = (period(-1 if side else 1), o)
                        list_send(j, piece, to, ring_op(step, half, side))

    def ring_end():
        for j in range(2):
            for side in range(2):
                sent[j, ring_op(3, side, side)].wait_recv()

    def partner_send(*steps):
        for step in steps:
            for j in range(2):
                list_send(j, pair[j].at[c, period(step)], (t, o + 1 - 2 * c), 32 + step % 8)

    def partner_take():
        for step in range(8):
            for j in range(2):
                sent[j, 32 + step].wait_recv()

    def own_rows():
        for start in (0, 256):
            widen(o, (pl.ds(start, 256),))

    def sort():
        lax.fori_loop(1, OWNERS, wait_list, 0)
        rows = sorted_terms(source[...], target[...], moment[...], block_lists[:, 0, :])
        for q, (meta_row, time_row) in enumerate(rows):
            meta[c, t, chip, pl.ds(q, 1), :] = meta_row
            time[c, t, chip, pl.ds(q, 1), :] = time_row

    def both(group, step, *numbers):
        for g in group:
            getattr(g, step)(*numbers)

    def run(order):
        for word in order:
            if word == "own":
                own_rows()
            elif word == "sort":
                sort()
            elif word == "plane":
                plane_send()
            elif word == "taken":
                plane_take()
            elif word == "end":
                ring_end()
            elif word == "partner":
                partner_take()
            elif word[0] == "R":
                ring_start(int(word[1]))
            elif word[0] == "P":
                partner_send(*(int(k) for k in word[1:].split(",")))
            else:
                numbers = [int(k) for k in word[2:].split(",") if k]
                step = STEPS[word[1]]
                if step == "shared" or not numbers:
                    both(big, step, *numbers)
                else:
                    for k in numbers:
                        both(big, step, k)

    run(ORDER)
    for g in big:
        g.finish()
    for copy in sent.values():
        copy.wait_send()


FAR_FIRST = (10, 6, 9, 11, 14, 2, 5, 7, 8, 13, 15, 1, 3, 4, 12, 0)
STEPS = {
    "b": "begin",
    "s": "own_second",
    "n": "near",
    "m": "near_second",
    "f": "far",
    "c": "column_near",
    "d": "column_far",
    "h": "shared",
}
ORDER = (
    "Mb", "own", "sort", "plane", "Ms", "Mn", "Mm", "taken", "R0", "P0", "Mf", "Mc0", "R1",
    "P1,-1", "Mc1", "Mh0,4,8", "R2", "P2,-2", "Mc2", "Mh1,2,12", "R3", "P3,-3", "Mc3",
    "Md0", "Mh5,6", "Md1", "Mh9,10", "end", "P4", "Md2", "Mh13,14", "Md3", "Mh3,7,11,15",
    "partner",
)

VMEM = pl.BlockSpec(memory_space=pltpu.VMEM)
HBM = pl.BlockSpec(memory_space=pltpu.HBM)


def in_hbm(*arrays):
    return [pltpu.with_memory_space_constraint(a, pltpu.HBM) for a in arrays]


def spread(*arrays):
    return pl.pallas_call(
        spread_kernel,
        out_shape=(
            jax.ShapeDtypeStruct((2 * OWNERS * ROWS, 128), F32),
            jax.ShapeDtypeStruct((2, PERIODS, OWNERS // 2, 8, 128), jnp.int32),
            jax.ShapeDtypeStruct((2, PERIODS, OWNERS // 2, 8, 128), F32),
        ),
        in_specs=[HBM] * 5,
        out_specs=[VMEM] * 3,
        scratch_shapes=[
            pltpu.VMEM((ROWS, WIDTH), F32),
            pltpu.VMEM((1, ROWS), jnp.int32),
            pltpu.VMEM((1, ROWS), jnp.int32),
            pltpu.VMEM((1, ROWS), F32),
            pltpu.VMEM((OWNERS, 1, 128), jnp.int32),
            pltpu.VMEM((OWNERS, ROWS, WIDTH), BF16),
            pltpu.VMEM((OWNERS, 1, 128), jnp.int32),
            pltpu.SemaphoreType.DMA((5,)),
            pltpu.SemaphoreType.DMA((2, 2 * Gather.OPS)),
            pltpu.SemaphoreType.DMA((2, OWNERS)),
            pltpu.SemaphoreType.DMA((2, 2, 40)),
        ],
        compiler_params=pltpu.CompilerParams(
            collective_id=0, has_side_effects=True, vmem_limit_bytes=28 * 2**20
        ),
        name="spread",
    )(*in_hbm(*arrays))


def message_kernel(
    wide, meta, time, freq_h, weight_h, bias_h, memory_h, totals, counts,
    freq, weight, bias, memory, windows, window_times, pieces, rows_v, rows_s, index_v, index_s,
    segments, parts, gathered, sem, index_sems, load_sems,
):
    t = lax.axis_index("tm")
    bucket = lax.axis_index("node") * PERIODS + t
    mine = pl.ds(pl.multiple_of(t * SHARE, SHARE), SHARE)
    loads = [
        pltpu.make_async_copy(src, dst, load_sems.at[i])
        for i, (src, dst) in enumerate(
            ((freq_h, freq), (weight_h, weight), (bias_h, bias), (memory_h.at[mine], memory))
        )
    ]
    for load in loads:
        load.start()
    totals[...] = jnp.zeros_like(totals)
    counts[...] = jnp.zeros_like(counts)
    gathered[...] = jnp.zeros_like(gathered)
    start_parts, end_parts = [], []
    for i in range(8):
        own = meta[pl.ds(32 * i, 32)] >> 20
        start_parts.append(jnp.sum(jnp.where(own < bucket, 1.0, 0.0), axis=1))
        end_parts.append(jnp.sum(jnp.where(own <= bucket, 1.0, 0.0), axis=1))
    ones_row = jnp.ones((8, 128), BF16)
    start = dot(ones_row, jnp.concatenate(start_parts, 0).astype(BF16), NT)
    end = dot(ones_row, jnp.concatenate(end_parts, 0).astype(BF16), NT)
    upper = where01(iota((BLOCKS, BLOCKS), 0) < iota((BLOCKS, BLOCKS), 1))
    ones_wide = jnp.ones((8, BLOCKS), BF16)
    ones_col = jnp.ones((BLOCKS, 128), BF16)
    ones_term = jnp.ones((CHUNK, 128), BF16)
    longest = jnp.max(end - start)
    for load in loads:
        load.wait()
    own_rows = memory[...].astype(BF16)
    own_rows = jnp.concatenate([own_rows, jnp.zeros((128 - SHARE, WIDTH), BF16)], 0)
    freqs = jnp.broadcast_to(freq[...], (CHUNK, 128))

    def index_copy(ch):
        return pltpu.make_async_copy(index_v.at[ch], index_s.at[ch], index_sems.at[ch])

    def one_round(r, carry):
        begin = start + (r * 128).astype(F32)
        size = jnp.clip(end - begin, 0.0, 128.0)
        before = dot(size.astype(BF16), upper)
        which = iota((8, BLOCKS), 0)
        begin_i = begin.astype(jnp.int32)
        rows_v[...] = jnp.where(which == 0, begin_i, (before + size).astype(jnp.int32))
        copy = pltpu.make_async_copy(rows_v, rows_s, sem)
        copy.start()
        copy.wait()
        total = rows_s[1, BLOCKS - 1]

        def fetch(i, carry):
            for u in range(8):
                b = i * 8 + u
                at = rows_s[0, b] >> 7
                for j in range(2):
                    from_row = pl.ds(jnp.minimum(at + j, 7), 1)
                    windows[j, pl.ds(b, 1), :] = meta[b, from_row, :]
                    window_times[j, pl.ds(b, 1), :] = time[b, from_row, :]
            return carry

        lax.fori_loop(0, BLOCKS // 8, fetch, 0)
        for j in range(2):
            m = windows[j]
            w = window_times[j]
            period = (iota((BLOCKS, 128), 0) >> 4) & 7
            seg = period * SHARE + ((m >> 14) & 63) - 256
            t1 = w.astype(BF16).astype(F32)
            t2 = (w - t1).astype(BF16).astype(F32)
            t3 = w - t1 - t2
            for k, piece in enumerate(
                (seg.astype(F32), ((m >> 6) & 255).astype(F32), (m & 63).astype(F32), t1, t2, t3)
            ):
                pieces[:, 256 * k + 128 * j : 256 * k + 128 * (j + 1)] = piece.astype(BF16)
        offset = (begin_i & 127).astype(F32) - before

        def one_group(group, carry):
            first = group * GROUP * CHUNK

            def locate(ch, carry):
                at = first + ch * CHUNK
                p = (at + iota((CHUNK, BLOCKS), 0)).astype(F32)
                low = jnp.broadcast_to(before[0:1], (CHUNK, BLOCKS))
                high = low + jnp.broadcast_to(size[0:1], (CHUNK, BLOCKS))
                hit = (low <= p) & (p < high)
                shift = jnp.sum(
                    jnp.where(hit, jnp.broadcast_to(offset[0:1], (CHUNK, BLOCKS)), 0.0),
                    axis=1,
                    keepdims=True,
                )
                found = dot(where01(hit), pieces[...])
                here = (p + shift) == iota((CHUNK, BLOCKS), 1).astype(F32)
                chosen = [
                    jnp.where(here, found[:, 256 * k : 256 * (k + 1)], 0.0).astype(BF16)
                    for k in range(6)
                ]
                other = dot(ones_wide, chosen[1], NT) * 64.0 + dot(ones_wide, chosen[2], NT)
                index_v[ch] = other.astype(jnp.int32) * 2
                index_copy(ch).start()
                seg_row = dot(ones_wide, chosen[0], NT) + 256.0
                lane_p = at + iota((8, CHUNK), 1)
                segments[ch] = jnp.where(lane_p < total, seg_row, -1.0)
                seg_col = dot(chosen[0], ones_col).astype(jnp.int32) + 256
                own_hot = where01((seg_col & 63) == iota((CHUNK, 128), 1))
                own = dot(own_hot, own_rows).astype(BF16)
                moment = (
                    dot(chosen[3], ones_col) + dot(chosen[4], ones_col) + dot(chosen[5], ones_col)
                )
                encoding = cosine(moment * freqs).astype(BF16)
                parts[ch] = dot(own, weight[pl.ds(0, WIDTH), :]) + dot(
                    encoding, weight[pl.ds(2 * WIDTH, 128), :]
                )
                parts[ch] = parts[ch] + bias[...]
                return carry

            def collect(ch, carry):
                index_copy(ch).wait()

                def pick(i, carry):
                    for u in range(UNROLL):
                        q = i * UNROLL + u
                        at = pl.multiple_of(index_s[ch, 0, q], 2)
                        gathered[pl.ds(2 * q, 2), :] = wide[pl.ds(at, 2), :]
                    return carry

                left = jnp.minimum(total - first - ch * CHUNK, CHUNK)
                lax.fori_loop(0, (left + UNROLL - 1) // UNROLL, pick, 0)
                other = sum(
                    dot(
                        gathered[pl.ds(side, CHUNK, stride=2), :].astype(BF16),
                        weight[pl.ds(WIDTH + 128 * side, 128), :],
                    )
                    for side in range(2)
                )
                message = jnp.maximum(parts[ch] + other, 0.0)
                seg_hot = where01(
                    iota((ROWS, CHUNK), 0).astype(F32)
                    == jnp.broadcast_to(segments[ch, 0:1, :], (ROWS, CHUNK))
                )
                upper_part = message.astype(BF16)
                lower_part = (message - upper_part.astype(F32)).astype(BF16)
                totals[...] += dot(seg_hot, upper_part) + dot(seg_hot, lower_part)
                counts[...] += dot(seg_hot, ones_term)
                return carry

            chunks = jnp.minimum((total - first + CHUNK - 1) // CHUNK, GROUP)
            lax.fori_loop(0, chunks, locate, 0)
            lax.fori_loop(0, chunks, collect, 0)
            return carry

        lax.fori_loop(0, (total + GROUP * CHUNK - 1) // (GROUP * CHUNK), one_group, 0)
        return carry

    rounds = (longest.astype(jnp.int32) + 127) // 128
    lax.fori_loop(0, rounds, one_round, 0)


def messages(wide, meta, time, *others):
    return pl.pallas_call(
        message_kernel,
        out_shape=(
            jax.ShapeDtypeStruct((ROWS, WIDTH), F32),
            jax.ShapeDtypeStruct((ROWS, 128), F32),
        ),
        in_specs=[VMEM] * 3 + [HBM] * 4,
        out_specs=[VMEM] * 2,
        scratch_shapes=[
            pltpu.VMEM((1, 128), F32),
            pltpu.VMEM((2 * WIDTH + 128, WIDTH), BF16),
            pltpu.VMEM((1, WIDTH), F32),
            pltpu.VMEM((SHARE, WIDTH), F32),
            pltpu.VMEM((2, BLOCKS, 128), jnp.int32),
            pltpu.VMEM((2, BLOCKS, 128), F32),
            pltpu.VMEM((BLOCKS, 6 * 256), BF16),
            pltpu.VMEM((8, BLOCKS), jnp.int32),
            pltpu.SMEM((8, BLOCKS), jnp.int32),
            pltpu.VMEM((GROUP, 8, CHUNK), jnp.int32),
            pltpu.SMEM((GROUP, 8, CHUNK), jnp.int32),
            pltpu.VMEM((GROUP, 8, CHUNK), F32),
            pltpu.VMEM((GROUP, CHUNK, WIDTH), F32),
            pltpu.VMEM((2 * CHUNK, 128), F32),
            pltpu.SemaphoreType.DMA,
            pltpu.SemaphoreType.DMA((GROUP,)),
            pltpu.SemaphoreType.DMA((4,)),
        ],
        compiler_params=pltpu.CompilerParams(vmem_limit_bytes=16 * 2**20),
        name="messages",
    )(wide, meta, time, *in_hbm(*others))


def update_kernel(
    totals, counts, weight, bias, memory_h, arrived, final, memory, history, load_sem, sems,
):
    t = lax.axis_index("tm")
    o = lax.axis_index("node")
    mine = pl.ds(pl.multiple_of(t * SHARE, SHARE), SHARE)
    load = pltpu.make_async_copy(memory_h.at[mine], memory, load_sem)
    load.start()
    barrier = pltpu.get_barrier_semaphore()
    for k in range(1, PERIODS):
        pl.semaphore_signal(
            barrier, inc=1, device_id=(lax.rem(t + k, PERIODS), o), device_id_type=MESH
        )
    count = counts[...]
    count = jnp.concatenate([count, count], 1)
    mean = (totals[...] / jnp.maximum(count, 1.0)).astype(BF16)
    gates = dot(mean, weight[...])
    rate = jax.nn.sigmoid(gates[:, :WIDTH] + bias[...])
    candidate = jnp.tanh(gates[:, WIDTH:])
    touched = count > 0.0
    keep = jnp.where(touched, 1.0 - rate, 1.0)
    write = jnp.where(touched, rate * candidate, 0.0)
    load.wait()
    state = memory[...]
    for k in range(PERIODS):
        rows = slice(k * SHARE, (k + 1) * SHARE)
        state = keep[rows] * state + write[rows]
        history[k] = state.astype(BF16)

        @pl.when(t == k)
        def _():
            final[...] = state

    pl.semaphore_wait(barrier, PERIODS - 1)
    copies = []
    for k in (4, 3, 5, 2, 6, 1, 7):
        to = lax.rem(t + k, PERIODS)
        copy = pltpu.make_async_remote_copy(
            src_ref=history.at[to],
            dst_ref=arrived.at[t],
            send_sem=sems.at[0, k],
            recv_sem=sems.at[1, k],
            device_id=(to, o),
            device_id_type=MESH,
        )
        copy.start()
        copies.append(copy)
    arrived[pl.ds(t, 1)] = history[pl.ds(t, 1)]
    for copy in copies:
        copy.wait()


def update(totals, counts, weight, bias, memory):
    return pl.pallas_call(
        update_kernel,
        out_shape=(
            jax.ShapeDtypeStruct((PERIODS, SHARE, WIDTH), BF16),
            jax.ShapeDtypeStruct((SHARE, WIDTH), F32),
        ),
        in_specs=[VMEM] * 4 + [HBM],
        out_specs=[VMEM] * 2,
        scratch_shapes=[
            pltpu.VMEM((SHARE, WIDTH), F32),
            pltpu.VMEM((PERIODS, SHARE, WIDTH), BF16),
            pltpu.SemaphoreType.DMA,
            pltpu.SemaphoreType.DMA((2, PERIODS)),
        ],
        compiler_params=pltpu.CompilerParams(
            collective_id=1, has_side_effects=True, vmem_limit_bytes=16 * 2**20
        ),
        name="update",
    )(totals, counts, weight, bias, *in_hbm(memory))


def shards(
    memory,
    src_slot,
    dst_slot,
    event_time,
    touched_rows,
    time_freq,
    msg_weight,
    msg_bias,
    gate_weight,
    update_bias,
):
    wide, meta, time = spread(
        memory,
        src_slot[0],
        dst_slot[0],
        event_time[0],
        touched_rows.reshape(OWNERS, 1, 128),
    )
    totals, counts = messages(
        wide,
        meta.reshape(BLOCKS, 8, 128),
        time.reshape(BLOCKS, 8, 128),
        time_freq[None],
        msg_weight,
        msg_bias[None],
        memory,
    )
    arrived, final = update(totals, counts, gate_weight, update_bias[None], memory)
    mine = lax.broadcasted_iota(jnp.int32, (PERIODS, SHARE, WIDTH), 0) == lax.axis_index("tm")
    result = jnp.where(mine, final[None], arrived.astype(F32))
    return result.reshape(1, ROWS, WIDTH)


def solution(mesh):
    return jax.shard_map(
        shards,
        mesh=mesh,
        in_specs=(
            P("node", None),
            P("tm", "node", None),
            P("tm", "node", None),
            P("tm", "node", None),
            P("tm", "node", None, None),
            P(),
            P(),
            P(),
            P(),
            P(),
        ),
        out_specs=P("tm", "node", None),
        check_vma=False,
    )
```

```python
import math

import jax
import jax.numpy as jnp
from jax import lax
from jax.experimental import pallas as pl
from jax.experimental.pallas import tpu as pltpu
from jax.sharding import PartitionSpec as P

MESH = pl.DeviceIdType.MESH
F32 = jnp.float32
BF16 = jnp.bfloat16
NT = (((1,), (1,)), ((), ()))
NN = (((1,), (0,)), ((), ()))

PERIODS = 8
OWNERS = 32
ROWS = 512
WIDTH = 256
TERMS = 1024
SHARE = ROWS // PERIODS
BLOCKS = PERIODS * OWNERS
CHUNK = 512
GROUP = 4
UNROLL = 32


def dot(a, b, dims=NN):
    return lax.dot_general(a, b, dims, preferred_element_type=F32)


def iota(shape, dim):
    return lax.broadcasted_iota(jnp.int32, shape, dim)


def where01(mask):
    return jnp.where(mask, 1.0, 0.0).astype(BF16)


def cosine(angle):
    turns = jnp.floor(angle * (0.5 / math.pi) + 0.5)
    rest = angle - turns * 6.28125
    rest = rest - turns * (2.0 * math.pi - 6.28125)
    square = rest * rest
    value = jnp.full_like(angle, 1.0 / math.factorial(16))
    for k in range(7, -1, -1):
        value = value * square + (-1.0) ** k / math.factorial(2 * k)
    return value


def slot_columns(sources, targets):
    lane = iota((TERMS, 128), 1)
    ones = jnp.ones((128, 128), BF16)
    square = iota((128, 128), 0) == iota((128, 128), 1)
    owners, places = [], []
    for slots in (sources, targets):
        for q in range(4):
            row = jnp.broadcast_to(slots[:, 128 * q : 128 * (q + 1)], (128, 128))
            owners.append(dot(jnp.where(square, row >> 7, 0).astype(F32).astype(BF16), ones))
            places.append(dot(jnp.where(square, row & 127, 0).astype(F32).astype(BF16), ones))
    owner = jnp.concatenate(owners, 0).astype(jnp.int32)
    slot = jnp.concatenate(places, 0).astype(jnp.int32)
    return owner, slot, where01(owner == lane)


def sorted_terms(owner, slot, owner_hot, times, lists):
    lane = iota((TERMS, 128), 1)
    ones = jnp.ones((128, 128), BF16)
    table = jnp.concatenate([(lists - 256).astype(F32), jnp.zeros((128 - OWNERS, 128), F32)], 0)
    per_owner = dot(owner_hot, table.astype(BF16))
    picked = jnp.where(slot == lane, per_owner, 0.0).astype(BF16)
    row = dot(picked, ones).astype(jnp.int32) + 256
    node = owner * ROWS + row
    bucket = (node >> 6).astype(F32)
    rest = (node & 63).astype(F32)
    eighth = jnp.full((8, 128), 1.0 / 128.0, BF16)
    bucket_row = dot(eighth, bucket.astype(BF16), NT)
    rest_row = dot(eighth, rest.astype(BF16), NT)
    key_col = bucket * TERMS + iota((TERMS, 128), 0).astype(F32)
    key_row = bucket_row * TERMS + iota((8, TERMS), 1).astype(F32)
    below = jnp.zeros((TERMS, 128), F32)
    for q in range(8):
        part = jnp.broadcast_to(key_row[0:1, 128 * q : 128 * (q + 1)], (TERMS, 128))
        below = below + jnp.where(part < key_col, 1.0, 0.0)
    place = dot(below.astype(BF16), ones).astype(jnp.int32)
    half = TERMS // 2
    other_bucket = jnp.concatenate([bucket_row[:, half:], bucket_row[:, :half]], 1)
    other_rest = jnp.concatenate([rest_row[:, half:], rest_row[:, :half]], 1)
    time = jnp.broadcast_to(jnp.concatenate([times, times], 1), (8, TERMS))
    t1 = time.astype(BF16).astype(F32)
    t2 = (time - t1).astype(BF16).astype(F32)
    t3 = time - t1 - t2
    which = iota((8, TERMS), 0)
    meta = jnp.zeros((8, TERMS), F32)
    for k, piece in enumerate((bucket_row, rest_row, other_bucket, other_rest, t1, t2, t3)):
        meta = jnp.where(which == k, piece, meta)
    meta = meta.astype(BF16)
    rows = []
    for q in range(8):
        out = dot(meta, where01(place == lane + 128 * q))
        whole = out.astype(jnp.int32)
        own = whole[0:1] * 64 + whole[1:2]
        other = whole[2:3] * 64 + whole[3:4]
        rows.append(((own << 14) | other, out[4:5] + out[5:6] + out[6:7]))
    return rows


class Gather:
    OPS = 36
    COLUMNS = ((0, 0), (1, -1), (2, 1), (3, 2))
    PLACES = (0, -1, 1, 2)

    def __init__(self, ref, start, size, first, base, sems, at, landed=None):
        self.ref = ref
        self.full = (pl.ds(start, size),)
        self.top = (pl.ds(start, size // 2),)
        self.bottom = (pl.ds(start + size // 2, size // 2),)
        self.first, self.base, self.sems, self.at = first, base, sems, at
        self.landed = landed
        self.started = {}

    def node(self, du, dv, flip=False):
        t, x, y, c = self.at
        dx, dy = (du, dv) if self.first == 0 else (dv, du)
        core = 1 - c if flip else c
        return (lax.rem(x + dx + 4, 4) * 4 + lax.rem(y + dy + 4, 4)) * 2 + core

    def land(self, du, dv, flip=False):
        if self.landed is not None:
            self.landed(self.node(du, dv, flip), self.full)

    def start(self, op, du, dv, part, to):
        piece = self.ref.at[(self.node(du, dv),) + part]
        copy = pltpu.make_async_remote_copy(
            src_ref=piece,
            dst_ref=piece,
            send_sem=self.sems.at[0, self.base + op],
            recv_sem=self.sems.at[1, self.base + op],
            device_id=(self.at[0], to),
            device_id_type=MESH,
        )
        copy.start()
        self.started[op] = copy

    def wait(self, op):
        self.started[op].wait_recv()

    def share(self, k, du, dv):
        self.start(20 + k, du, dv, self.full, self.node(0, 0, True))

    def second(self, i, du):
        self.start(4 + 4 * i, du, 0, self.full, self.node(0, 1))
        self.start(5 + 4 * i, du, 0, self.full, self.node(0, -1))
        self.share(4 * i, du, 0)

    def begin(self):
        self.start(0, 0, 0, self.full, self.node(1, 0))
        self.start(1, 0, 0, self.full, self.node(-1, 0))

    def own_second(self):
        self.second(0, 0)

    def near(self):
        self.wait(0)
        self.start(2, -1, 0, self.top, self.node(1, 0))
        self.wait(1)
        self.start(3, 1, 0, self.bottom, self.node(-1, 0))
        self.second(1, -1)

    def near_second(self):
        self.second(2, 1)
        self.land(-1, 0)
        self.land(1, 0)

    def far(self):
        self.wait(2)
        self.wait(3)
        self.second(3, 2)
        self.land(2, 0)

    def column_near(self, i):
        du = self.PLACES[i]
        self.wait(4 + 4 * i)
        self.start(6 + 4 * i, du, -1, self.top, self.node(0, 1))
        self.share(4 * i + 1, du, -1)
        self.wait(5 + 4 * i)
        self.start(7 + 4 * i, du, 1, self.bottom, self.node(0, -1))
        self.share(4 * i + 2, du, 1)
        self.land(du, -1)
        self.land(du, 1)

    def column_far(self, i):
        du = self.PLACES[i]
        self.wait(6 + 4 * i)
        self.wait(7 + 4 * i)
        self.share(4 * i + 3, du, 2)
        self.land(du, 2)

    def shared(self, *ks):
        for k in ks:
            self.wait(20 + k)
            self.land(self.PLACES[k // 4], self.PLACES[k % 4], True)

    def finish(self):
        for copy in self.started.values():
            copy.wait_send()


def spread_kernel(
    memory_h, source_h, target_h, moment_h, lists_h, wide, meta, time,
    memory, source, target, moment, lists, table, block_lists, owner_v, slot_v, owner_hot_v, load_sems, sems, list_sems, share_sems,
):
    t = lax.axis_index("tm")
    o = lax.axis_index("node")
    x, y, c = o // 8, lax.rem(o // 2, 4), lax.rem(o, 2)
    at = (t, x, y, c)
    loads = [
        pltpu.make_async_copy(src, dst, load_sems.at[i])
        for i, (src, dst) in enumerate(
            (
                (memory_h, memory),
                (lists_h, lists),
                (source_h, source),
                (target_h, target),
                (moment_h, moment),
            )
        )
    ]
    for load in loads:
        load.start()
    barrier = pltpu.get_barrier_semaphore()

    def greet(k, carry):
        pl.semaphore_signal(
            barrier, inc=1, device_id=(t, lax.rem(o + k, OWNERS)), device_id_type=MESH
        )
        return carry

    def greet_periods(k, carry):
        pl.semaphore_signal(
            barrier, inc=1, device_id=(lax.rem(t + k, PERIODS), o), device_id_type=MESH
        )
        return carry

    lax.fori_loop(1, OWNERS, greet, 0)
    lax.fori_loop(1, PERIODS, greet_periods, 0)
    for load in loads:
        load.wait()
    table[pl.ds(o, 1)] = memory[...].astype(BF16)[None]
    block_lists[pl.ds(o, 1)] = lists[pl.ds(o, 1)]

    def widen(node, part):
        rows = part[0]
        piece = table[node, rows, :].astype(F32)
        first = pl.multiple_of((node * ROWS + rows.start) * 2, 128)
        for side in range(2):
            wide[pl.ds(first + side, rows.size, stride=2), :] = piece[:, 128 * side : 128 * side + 128]

    pl.semaphore_wait(barrier, OWNERS - 1 + PERIODS - 1)

    def list_copy(k):
        to = lax.rem(o + k, OWNERS)
        return pltpu.make_async_remote_copy(
            src_ref=lists.at[to],
            dst_ref=block_lists.at[o],
            send_sem=list_sems.at[0, k],
            recv_sem=list_sems.at[1, k],
            device_id=(t, to),
            device_id_type=MESH,
        )

    def wait_list(k, carry):
        list_copy(k).wait()
        return carry

    for k in FAR_FIRST:
        for core in range(2):
            if k + core:
                list_copy(2 * k + core).start()
    n = Gather.OPS
    big = (
        Gather(table, 0, 256, 0, 0, sems, at, widen),
        Gather(table, 256, 256, 1, n, sems, at, widen),
    )
    chip = o // 2
    pair = (meta, time)

    def list_send(j, piece, to, op):
        copy = pltpu.make_async_remote_copy(
            src_ref=piece,
            dst_ref=piece,
            send_sem=share_sems.at[0, j, op],
            recv_sem=share_sems.at[1, j, op],
            device_id=to,
            device_id_type=MESH,
        )
        copy.start()
        sent[j, op] = copy

    sent = {}

    def plane_send():
        for k in FAR_FIRST[:-1]:
            to = lax.rem(chip + k, 16) * 2 + c
            for j in range(2):
                list_send(j, pair[j].at[c, t, chip], (t, to), k)

    def plane_take():
        for k in range(1, 16):
            for j in range(2):
                sent[j, k].wait_recv()

    def period(step):
        return lax.rem(t + step + PERIODS, PERIODS)

    def ring_op(step, half, side):
        return 16 + 4 * step + 2 * half + side

    def ring_start(step):
        for j in range(2):
            for half in range(2):
                for side in range(2):
                    if step:
                        sent[j, ring_op(step - 1, half, side)].wait_recv()
                    if step < 3 or half == side:
                        piece = pair[j].at[c, period(step if side else -step), pl.ds(8 * half, 8)]
                        to = (period(-1 if side else 1), o)
                        list_send(j, piece, to, ring_op(step, half, side))

    def ring_end():
        for j in range(2):
            for side in range(2):
                sent[j, ring_op(3, side, side)].wait_recv()

    def partner_send(*steps):
        for step in steps:
            for j in range(2):
                list_send(j, pair[j].at[c, period(step)], (t, o + 1 - 2 * c), 32 + step % 8)

    def partner_take():
        for step in range(8):
            for j in range(2):
                sent[j, 32 + step].wait_recv()

    def own_rows():
        for start in (0, 256):
            widen(o, (pl.ds(start, 256),))

    def sort():
        columns = slot_columns(source[...], target[...])
        owner_v[...], slot_v[...], owner_hot_v[...] = columns
        lax.fori_loop(1, OWNERS, wait_list, 0)
        rows = sorted_terms(
            owner_v[...], slot_v[...], owner_hot_v[...], moment[...], block_lists[:, 0, :]
        )
        for q, (meta_row, time_row) in enumerate(rows):
            meta[c, t, chip, pl.ds(q, 1), :] = meta_row
            time[c, t, chip, pl.ds(q, 1), :] = time_row

    def both(group, step, *numbers):
        for g in group:
            getattr(g, step)(*numbers)

    def run(order):
        for word in order:
            if word == "own":
                own_rows()
            elif word == "sort":
                sort()
            elif word == "plane":
                plane_send()
            elif word == "taken":
                plane_take()
            elif word == "end":
                ring_end()
            elif word == "partner":
                partner_take()
            elif word[0] == "R":
                ring_start(int(word[1]))
            elif word[0] == "P":
                partner_send(*(int(k) for k in word[1:].split(",")))
            else:
                numbers = [int(k) for k in word[2:].split(",") if k]
                step = STEPS[word[1]]
                if step == "shared" or not numbers:
                    both(big, step, *numbers)
                else:
                    for k in numbers:
                        both(big, step, k)

    run(ORDER)
    for g in big:
        g.finish()
    for copy in sent.values():
        copy.wait_send()


FAR_FIRST = (10, 6, 9, 11, 14, 2, 5, 7, 8, 13, 15, 1, 3, 4, 12, 0)
STEPS = {
    "b": "begin",
    "s": "own_second",
    "n": "near",
    "m": "near_second",
    "f": "far",
    "c": "column_near",
    "d": "column_far",
    "h": "shared",
}
ORDER = (
    "Mb", "Ms", "own", "sort", "plane", "Mn", "Mm", "taken", "R0", "Mf", "Mc0", "P0", "R1",
    "Mc1", "P1,-1", "Mh0,4,8", "R2", "Mc2", "P2,-2", "Mh1,2,12", "R3", "Mc3", "Md0",
    "P3,-3", "Mh5,6", "Md1", "Mh9,10", "Md2", "end", "P4", "Mh13,14", "Md3", "Mh3,7,11,15",
    "partner",
)

VMEM = pl.BlockSpec(memory_space=pltpu.VMEM)
HBM = pl.BlockSpec(memory_space=pltpu.HBM)


def in_hbm(*arrays):
    return [pltpu.with_memory_space_constraint(a, pltpu.HBM) for a in arrays]


def spread(*arrays):
    return pl.pallas_call(
        spread_kernel,
        out_shape=(
            jax.ShapeDtypeStruct((2 * OWNERS * ROWS, 128), F32),
            jax.ShapeDtypeStruct((2, PERIODS, OWNERS // 2, 8, 128), jnp.int32),
            jax.ShapeDtypeStruct((2, PERIODS, OWNERS // 2, 8, 128), F32),
        ),
        in_specs=[HBM] * 5,
        out_specs=[VMEM] * 3,
        scratch_shapes=[
            pltpu.VMEM((ROWS, WIDTH), F32),
            pltpu.VMEM((1, ROWS), jnp.int32),
            pltpu.VMEM((1, ROWS), jnp.int32),
            pltpu.VMEM((1, ROWS), F32),
            pltpu.VMEM((OWNERS, 1, 128), jnp.int32),
            pltpu.VMEM((OWNERS, ROWS, WIDTH), BF16),
            pltpu.VMEM((OWNERS, 1, 128), jnp.int32),
            pltpu.VMEM((TERMS, 128), jnp.int32),
            pltpu.VMEM((TERMS, 128), jnp.int32),
            pltpu.VMEM((TERMS, 128), BF16),
            pltpu.SemaphoreType.DMA((5,)),
            pltpu.SemaphoreType.DMA((2, 2 * Gather.OPS)),
            pltpu.SemaphoreType.DMA((2, OWNERS)),
            pltpu.SemaphoreType.DMA((2, 2, 40)),
        ],
        compiler_params=pltpu.CompilerParams(
            collective_id=0, has_side_effects=True, vmem_limit_bytes=28 * 2**20
        ),
        name="spread",
    )(*in_hbm(*arrays))


def message_kernel(
    wide, meta, time, freq_h, weight_h, bias_h, memory_h, totals, counts,
    freq, weight, bias, memory, windows, window_times, pieces, rows_v, rows_s, index_v, index_s,
    segments, parts, gathered, sem, index_sems, load_sems,
):
    t = lax.axis_index("tm")
    bucket = lax.axis_index("node") * PERIODS + t
    mine = pl.ds(pl.multiple_of(t * SHARE, SHARE), SHARE)
    loads = [
        pltpu.make_async_copy(src, dst, load_sems.at[i])
        for i, (src, dst) in enumerate(
            ((freq_h, freq), (weight_h, weight), (bias_h, bias), (memory_h.at[mine], memory))
        )
    ]
    for load in loads:
        load.start()
    totals[...] = jnp.zeros_like(totals)
    counts[...] = jnp.zeros_like(counts)
    gathered[...] = jnp.zeros_like(gathered)
    start_parts, end_parts = [], []
    for i in range(8):
        own = meta[pl.ds(32 * i, 32)] >> 20
        start_parts.append(jnp.sum(jnp.where(own < bucket, 1.0, 0.0), axis=1))
        end_parts.append(jnp.sum(jnp.where(own <= bucket, 1.0, 0.0), axis=1))
    ones_row = jnp.ones((8, 128), BF16)
    start = dot(ones_row, jnp.concatenate(start_parts, 0).astype(BF16), NT)
    end = dot(ones_row, jnp.concatenate(end_parts, 0).astype(BF16), NT)
    upper = where01(iota((BLOCKS, BLOCKS), 0) < iota((BLOCKS, BLOCKS), 1))
    ones_wide = jnp.ones((8, BLOCKS), BF16)
    ones_col = jnp.ones((BLOCKS, 128), BF16)
    ones_term = jnp.ones((CHUNK, 128), BF16)
    longest = jnp.max(end - start)
    for load in loads:
        load.wait()
    own_rows = memory[...].astype(BF16)
    own_rows = jnp.concatenate([own_rows, jnp.zeros((128 - SHARE, WIDTH), BF16)], 0)
    freqs = jnp.broadcast_to(freq[...], (CHUNK, 128))

    def index_copy(ch):
        return pltpu.make_async_copy(index_v.at[ch], index_s.at[ch], index_sems.at[ch])

    def one_round(r, carry):
        begin = start + (r * 128).astype(F32)
        size = jnp.clip(end - begin, 0.0, 128.0)
        before = dot(size.astype(BF16), upper)
        which = iota((8, BLOCKS), 0)
        begin_i = begin.astype(jnp.int32)
        rows_v[...] = jnp.where(which == 0, begin_i, (before + size).astype(jnp.int32))
        copy = pltpu.make_async_copy(rows_v, rows_s, sem)
        copy.start()
        copy.wait()
        total = rows_s[1, BLOCKS - 1]

        def fetch(i, carry):
            for u in range(8):
                b = i * 8 + u
                at = rows_s[0, b] >> 7
                for j in range(2):
                    from_row = pl.ds(jnp.minimum(at + j, 7), 1)
                    windows[j, pl.ds(b, 1), :] = meta[b, from_row, :]
                    window_times[j, pl.ds(b, 1), :] = time[b, from_row, :]
            return carry

        lax.fori_loop(0, BLOCKS // 8, fetch, 0)
        for j in range(2):
            m = windows[j]
            w = window_times[j]
            period = (iota((BLOCKS, 128), 0) >> 4) & 7
            seg = period * SHARE + ((m >> 14) & 63) - 256
            t1 = w.astype(BF16).astype(F32)
            t2 = (w - t1).astype(BF16).astype(F32)
            t3 = w - t1 - t2
            for k, piece in enumerate(
                (seg.astype(F32), ((m >> 6) & 255).astype(F32), (m & 63).astype(F32), t1, t2, t3)
            ):
                pieces[:, 256 * k + 128 * j : 256 * k + 128 * (j + 1)] = piece.astype(BF16)
        offset = (begin_i & 127).astype(F32) - before

        def one_group(group, carry):
            first = group * GROUP * CHUNK

            def locate(ch, carry):
                at = first + ch * CHUNK
                p = (at + iota((CHUNK, BLOCKS), 0)).astype(F32)
                low = jnp.broadcast_to(before[0:1], (CHUNK, BLOCKS))
                high = low + jnp.broadcast_to(size[0:1], (CHUNK, BLOCKS))
                hit = (low <= p) & (p < high)
                shift = jnp.sum(
                    jnp.where(hit, jnp.broadcast_to(offset[0:1], (CHUNK, BLOCKS)), 0.0),
                    axis=1,
                    keepdims=True,
                )
                found = dot(where01(hit), pieces[...])
                here = (p + shift) == iota((CHUNK, BLOCKS), 1).astype(F32)
                chosen = [
                    jnp.where(here, found[:, 256 * k : 256 * (k + 1)], 0.0).astype(BF16)
                    for k in range(6)
                ]
                other = dot(ones_wide, chosen[1], NT) * 64.0 + dot(ones_wide, chosen[2], NT)
                index_v[ch] = other.astype(jnp.int32) * 2
                index_copy(ch).start()
                seg_row = dot(ones_wide, chosen[0], NT) + 256.0
                lane_p = at + iota((8, CHUNK), 1)
                segments[ch] = jnp.where(lane_p < total, seg_row, -1.0)
                seg_col = dot(chosen[0], ones_col).astype(jnp.int32) + 256
                own_hot = where01((seg_col & 63) == iota((CHUNK, 128), 1))
                own = dot(own_hot, own_rows).astype(BF16)
                moment = (
                    dot(chosen[3], ones_col) + dot(chosen[4], ones_col) + dot(chosen[5], ones_col)
                )
                encoding = cosine(moment * freqs).astype(BF16)
                parts[ch] = dot(own, weight[pl.ds(0, WIDTH), :]) + dot(
                    encoding, weight[pl.ds(2 * WIDTH, 128), :]
                )
                parts[ch] = parts[ch] + bias[...]
                return carry

            def collect(ch, carry):
                index_copy(ch).wait()

                def pick(i, carry):
                    for u in range(UNROLL):
                        q = i * UNROLL + u
                        at = pl.multiple_of(index_s[ch, 0, q], 2)
                        gathered[pl.ds(2 * q, 2), :] = wide[pl.ds(at, 2), :]
                    return carry

                left = jnp.minimum(total - first - ch * CHUNK, CHUNK)
                lax.fori_loop(0, (left + UNROLL - 1) // UNROLL, pick, 0)
                other = sum(
                    dot(
                        gathered[pl.ds(side, CHUNK, stride=2), :].astype(BF16),
                        weight[pl.ds(WIDTH + 128 * side, 128), :],
                    )
                    for side in range(2)
                )
                message = jnp.maximum(parts[ch] + other, 0.0)
                seg_hot = where01(
                    iota((ROWS, CHUNK), 0).astype(F32)
                    == jnp.broadcast_to(segments[ch, 0:1, :], (ROWS, CHUNK))
                )
                upper_part = message.astype(BF16)
                lower_part = (message - upper_part.astype(F32)).astype(BF16)
                totals[...] += dot(seg_hot, upper_part) + dot(seg_hot, lower_part)
                counts[...] += dot(seg_hot, ones_term)
                return carry

            chunks = jnp.minimum((total - first + CHUNK - 1) // CHUNK, GROUP)
            lax.fori_loop(0, chunks, locate, 0)
            lax.fori_loop(0, chunks, collect, 0)
            return carry

        lax.fori_loop(0, (total + GROUP * CHUNK - 1) // (GROUP * CHUNK), one_group, 0)
        return carry

    rounds = (longest.astype(jnp.int32) + 127) // 128
    lax.fori_loop(0, rounds, one_round, 0)


def messages(wide, meta, time, *others):
    return pl.pallas_call(
        message_kernel,
        out_shape=(
            jax.ShapeDtypeStruct((ROWS, WIDTH), F32),
            jax.ShapeDtypeStruct((ROWS, 128), F32),
        ),
        in_specs=[VMEM] * 3 + [HBM] * 4,
        out_specs=[VMEM] * 2,
        scratch_shapes=[
            pltpu.VMEM((1, 128), F32),
            pltpu.VMEM((2 * WIDTH + 128, WIDTH), BF16),
            pltpu.VMEM((1, WIDTH), F32),
            pltpu.VMEM((SHARE, WIDTH), F32),
            pltpu.VMEM((2, BLOCKS, 128), jnp.int32),
            pltpu.VMEM((2, BLOCKS, 128), F32),
            pltpu.VMEM((BLOCKS, 6 * 256), BF16),
            pltpu.VMEM((8, BLOCKS), jnp.int32),
            pltpu.SMEM((8, BLOCKS), jnp.int32),
            pltpu.VMEM((GROUP, 8, CHUNK), jnp.int32),
            pltpu.SMEM((GROUP, 8, CHUNK), jnp.int32),
            pltpu.VMEM((GROUP, 8, CHUNK), F32),
            pltpu.VMEM((GROUP, CHUNK, WIDTH), F32),
            pltpu.VMEM((2 * CHUNK, 128), F32),
            pltpu.SemaphoreType.DMA,
            pltpu.SemaphoreType.DMA((GROUP,)),
            pltpu.SemaphoreType.DMA((4,)),
        ],
        compiler_params=pltpu.CompilerParams(vmem_limit_bytes=16 * 2**20),
        name="messages",
    )(wide, meta, time, *in_hbm(*others))


def update_kernel(
    totals, counts, weight, bias, memory_h, arrived, final, memory, history, load_sem, sems,
):
    t = lax.axis_index("tm")
    o = lax.axis_index("node")
    mine = pl.ds(pl.multiple_of(t * SHARE, SHARE), SHARE)
    load = pltpu.make_async_copy(memory_h.at[mine], memory, load_sem)
    load.start()
    barrier = pltpu.get_barrier_semaphore()
    for k in range(1, PERIODS):
        pl.semaphore_signal(
            barrier, inc=1, device_id=(lax.rem(t + k, PERIODS), o), device_id_type=MESH
        )
    count = counts[...]
    count = jnp.concatenate([count, count], 1)
    mean = (totals[...] / jnp.maximum(count, 1.0)).astype(BF16)
    gates = dot(mean, weight[...])
    rate = jax.nn.sigmoid(gates[:, :WIDTH] + bias[...])
    candidate = jnp.tanh(gates[:, WIDTH:])
    touched = count > 0.0
    keep = jnp.where(touched, 1.0 - rate, 1.0)
    write = jnp.where(touched, rate * candidate, 0.0)
    load.wait()
    state = memory[...]
    for k in range(PERIODS):
        rows = slice(k * SHARE, (k + 1) * SHARE)
        state = keep[rows] * state + write[rows]
        history[k] = state.astype(BF16)

        @pl.when(t == k)
        def _():
            final[...] = state

    pl.semaphore_wait(barrier, PERIODS - 1)
    copies = []
    for k in (4, 3, 5, 2, 6, 1, 7):
        to = lax.rem(t + k, PERIODS)
        copy = pltpu.make_async_remote_copy(
            src_ref=history.at[to],
            dst_ref=arrived.at[t],
            send_sem=sems.at[0, k],
            recv_sem=sems.at[1, k],
            device_id=(to, o),
            device_id_type=MESH,
        )
        copy.start()
        copies.append(copy)
    arrived[pl.ds(t, 1)] = history[pl.ds(t, 1)]
    for copy in copies:
        copy.wait()


def update(totals, counts, weight, bias, memory):
    return pl.pallas_call(
        update_kernel,
        out_shape=(
            jax.ShapeDtypeStruct((PERIODS, SHARE, WIDTH), BF16),
            jax.ShapeDtypeStruct((SHARE, WIDTH), F32),
        ),
        in_specs=[VMEM] * 4 + [HBM],
        out_specs=[VMEM] * 2,
        scratch_shapes=[
            pltpu.VMEM((SHARE, WIDTH), F32),
            pltpu.VMEM((PERIODS, SHARE, WIDTH), BF16),
            pltpu.SemaphoreType.DMA,
            pltpu.SemaphoreType.DMA((2, PERIODS)),
        ],
        compiler_params=pltpu.CompilerParams(
            collective_id=1, has_side_effects=True, vmem_limit_bytes=16 * 2**20
        ),
        name="update",
    )(totals, counts, weight, bias, *in_hbm(memory))


def shards(
    memory,
    src_slot,
    dst_slot,
    event_time,
    touched_rows,
    time_freq,
    msg_weight,
    msg_bias,
    gate_weight,
    update_bias,
):
    wide, meta, time = spread(
        memory,
        src_slot[0],
        dst_slot[0],
        event_time[0],
        touched_rows.reshape(OWNERS, 1, 128),
    )
    totals, counts = messages(
        wide,
        meta.reshape(BLOCKS, 8, 128),
        time.reshape(BLOCKS, 8, 128),
        time_freq[None],
        msg_weight,
        msg_bias[None],
        memory,
    )
    arrived, final = update(totals, counts, gate_weight, update_bias[None], memory)
    mine = lax.broadcasted_iota(jnp.int32, (PERIODS, SHARE, WIDTH), 0) == lax.axis_index("tm")
    result = jnp.where(mine, final[None], arrived.astype(F32))
    return result.reshape(1, ROWS, WIDTH)


def solution(mesh):
    return jax.shard_map(
        shards,
        mesh=mesh,
        in_specs=(
            P("node", None),
            P("tm", "node", None),
            P("tm", "node", None),
            P("tm", "node", None),
            P("tm", "node", None, None),
            P(),
            P(),
            P(),
            P(),
            P(),
        ),
        out_specs=P("tm", "node", None),
        check_vma=False,
    )
```
